256 devices in a mesh: dp: 4 (over z_lo, core), mp: 64 (over x, y, z_hi).
Axes of the slice: x: 4, y: 4, z: 8 (z_hi: 4, z_lo: 2; z = z_hi * 2 + z_lo), core: 2. Of those that a mesh axis runs over, the one named last changes fastest.
Arguments:
- tokens: bfloat16 [10240, 1792], P(('dp', 'mp')), may hold values from -6 to 6
- norm_gain: float32 [1792], replicated, may hold values from 0.5 to 1.5
- norm_bias: float32 [1792], replicated, may hold values from -3 to 3
- w_in: bfloat16 [1792, 15360], P('dp', 'mp'), may hold values from -0.125 to 0.125
- b_in: float32 [15360], P('mp'), may hold values from -3 to 3
- w_out: bfloat16 [15360, 1792], P('mp', 'dp'), may hold values from -0.046875 to 0.046875
- b_out: float32 [1792], replicated, may hold values from -3 to 3
Outputs:
- result: bfloat16 [10240, 1792], P(('dp', 'mp'))
The draws below stay inside these ranges and needn't reach their ends.
All inputs are finite; a program needn't handle non-finite values.
Results may differ from the reference program's by a relative error of at most 0.0042.
Values may be sent and summed in bfloat16 or wider, within the bound.
No kernel may reach another device: no remote copies, remote signals or barrier semaphores. Data moves between devices by JAX's collectives and lax.ppermute only.
A program may use at most 128 MiB of HBM per device.

```python
import jax
import jax.numpy as jnp
from jax import lax

D = 1792
FF = 15360
TOK_DEV = 40
TOKENS = 10240
N_MP = 64


def block_scale(rng, dims, pieces, low, top_value):
    level, own = 1.0, jax.random.fold_in(rng, 6)
    for axis_at, shards_of in pieces:
        draws = jnp.exp(jax.random.uniform(jax.random.fold_in(own, axis_at), (shards_of,), jnp.float32, low / len(pieces), top_value / len(pieces)))
        level = level * jnp.repeat(draws, dims[axis_at] // shards_of).reshape([-1 if axis == axis_at else 1 for axis in range(len(dims))])
    return level


def scatter_about(own_key, extent, scale, limit, split=(), dtype=jnp.bfloat16):
    array = scale * jax.random.normal(own_key, extent, jnp.float32)
    if split:
        array = array * block_scale(own_key, extent, split, -0.22, 0.18)
    return jnp.clip(array, -limit, limit).astype(dtype)


def setup_inputs(seed: int = 0) -> dict:
    streams_of = jax.random.split(jax.random.key(seed), 8)
    return {
        "tokens": scatter_about(streams_of[0], (TOKENS, D), 1.0, 6.0, ((0, 256),)),
        "norm_gain": jnp.clip(jax.random.uniform(streams_of[1], (D,), jnp.float32, 0.5, 1.5), 0.5, 1.5),
        "norm_bias": scatter_about(streams_of[2], (D,), 0.5, 3.0, (), jnp.float32),
        "w_in": scatter_about(streams_of[3], (D, FF), D ** -0.5, 0.125, ((0, 4), (1, 64))),
        "b_in": scatter_about(streams_of[4], (FF,), 0.5, 3.0, ((0, 64),), jnp.float32),
        "w_out": scatter_about(streams_of[5], (FF, D), FF ** -0.5, 0.046875, ((0, 64), (1, 4))),
        "b_out": scatter_about(streams_of[6], (D,), 0.5, 3.0, (), jnp.float32),
    }


def block_rows(rows, norm_gain, norm_bias, w_in, b_in, w_out, b_out):
    values = rows.astype(jnp.float32)
    center = lax.optimization_barrier(jnp.mean(values, axis=1, keepdims=True))
    spread = lax.optimization_barrier(jnp.mean((values - center) ** 2, axis=1, keepdims=True))
    normed = ((values - center) / jnp.sqrt(spread + 1e-06) * norm_gain + norm_bias).astype(jnp.bfloat16)
    pre = jnp.dot(normed, w_in, preferred_element_type=jnp.float32) + b_in
    hidden = jax.nn.gelu(pre, approximate=False).astype(jnp.bfloat16)
    summed = jnp.dot(hidden, w_out, preferred_element_type=jnp.float32)
    return (values + summed + b_out).astype(jnp.bfloat16)

def reference(tokens, norm_gain, norm_bias, w_in, b_in, w_out, b_out):
    group = TOK_DEV * N_MP
    blocks = tokens.reshape(TOKENS // group, group, D)
    done = lax.map(lambda rows: block_rows(rows, norm_gain, norm_bias, w_in, b_in, w_out, b_out), blocks)
    return done.reshape(TOKENS, D)
```

```python
import functools

import jax
import jax.numpy as jnp
from jax import lax
from jax.experimental import pallas as pl
from jax.experimental.pallas import tpu as pltpu
from jax.sharding import Mesh
from jax.sharding import PartitionSpec as P

AXES = ("zl", "c", "x", "y", "zh")
MP = ("x", "y", "zh")
DP = ("zl", "c")
Z = ("zl", "zh")
F32, BF16 = jnp.float32, jnp.bfloat16


def z_index(z):
    return (z % 2) * 4 + (z % 8) // 2


def z_perm(k):
    pairs = []
    for z in range(8):
        source = z + k if z % 2 == 0 else z - k
        pairs.append((z_index(source), z_index(z)))
    return pairs


def towards(array):
    return lax.ppermute(array, Z, z_perm(1))


def away(array):
    return lax.ppermute(array, Z, z_perm(-1))


def other_core(array):
    return lax.ppermute(array, "c", [(0, 1), (1, 0)])


def from_step(array, axis, k):
    return lax.ppermute(array, axis, [((i + k) % 4, i) for i in range(4)])


def to_step(array, axis, k):
    return lax.ppermute(array, axis, [(i, (i + k) % 4) for i in range(4)])


def gelu(value):
    return 0.5 * value * (1.0 + lax.erf(value * 0.7071067811865476))


def vmem():
    return pl.BlockSpec(memory_space=pltpu.VMEM)


def hidden_body(near_ref, far_ref, w0, w1, w2, w3, bias_ref, out_ref, pre_ref):
    pre_ref[...] = (
        jnp.dot(near_ref[...], jnp.concatenate([w0[...], w1[...]], 0), preferred_element_type=F32)
        + jnp.dot(far_ref[...], jnp.concatenate([w2[...], w3[...]], 0), preferred_element_type=F32)
    )
    bias = bias_ref[...]

    @pl.loop(0, 40)
    def _(i):
        rows = pl.ds(pl.multiple_of(i * 16, 16), 16)
        out_ref[rows, :] = gelu(pre_ref[rows, :] + bias).astype(BF16)


def hidden_of(near, far, w, bias):
    rows, cols = near.shape[0], w[0].shape[1]
    return pl.pallas_call(
        hidden_body,
        out_shape=jax.ShapeDtypeStruct((rows, cols), BF16),
        in_specs=[vmem()] * 7,
        out_specs=vmem(),
        scratch_shapes=[pltpu.VMEM((rows, cols), F32)],
    )(near, far, *w, bias)


def terms_body(x_first, h0, h1, h2, h3, w0, w1, w2, w3, own, s1, s2, s3, sums):
    total = jnp.dot(h0[...], w0[...], preferred_element_type=F32)
    for h, w in ((h1, w1), (h2, w2), (h3, w3)):
        total += jnp.dot(h[...], w[...], preferred_element_type=F32)
    sums[...] = total
    for k, ref in enumerate((own, s1, s2, s3)):
        for m in range(4):
            at = (m * 4 + k if x_first else k * 4 + m) * 40
            ref[m * 40 : m * 40 + 40, :] = sums[at : at + 40, :].astype(ref.dtype)


def terms_of(h, w, x_first):
    rows, cols = h[0].shape[0], w[0].shape[1]
    quarter = rows // 4
    return pl.pallas_call(
        functools.partial(terms_body, x_first),
        out_shape=[jax.ShapeDtypeStruct((quarter, cols), F32)]
        + [jax.ShapeDtypeStruct((quarter, cols), BF16)] * 3,
        in_specs=[vmem()] * 8,
        out_specs=[vmem()] * 4,
        scratch_shapes=[pltpu.VMEM((rows, cols), F32)],
    )(*h, *w)


def reduced(h, w, x_first):
    first, second = ("x", "y") if x_first else ("y", "x")
    own, *sent = terms_of(h, w, x_first)
    for k, piece in enumerate(sent):
        own = own + to_step(piece, first, k + 1).astype(F32)
    total = own[:40]
    for k in range(1, 4):
        total = total + to_step(own[k * 40 : k * 40 + 40].astype(BF16), second, k).astype(F32)
    return total


def swap_if(flag, a, b):
    return jnp.where(flag, b, a), jnp.where(flag, a, b)


def on_device(tokens, norm_gain, norm_bias, w_in, b_in, w_out, b_out):
    zl, core = lax.axis_index("zl") == 1, lax.axis_index("c") == 1
    ring = {}
    for name, own in (("in", w_in), ("out", w_out)):
        got = {0: own, 1: towards(own), -1: away(own)}
        got[2], got[-2] = towards(got[-1]), away(got[1])
        got[3], got[-3] = towards(got[-2]), away(got[2])
        got[4] = towards(got[-3])
        ring[name] = {k: (v, other_core(v)) for k, v in got.items()}
    bias = b_in.reshape(1, -1)
    biases = [bias] + [lax.ppermute(bias, Z, z_perm(k)) for k in (2, -2, 4)]
    groups = ((0, 1), (2, 3), (-2, -1), (4, -3))

    values = tokens.astype(F32)
    center = jnp.mean(values, axis=1, keepdims=True)
    spread = jnp.mean((values - center) ** 2, axis=1, keepdims=True)
    normed = ((values - center) / jnp.sqrt(spread + 1e-06) * norm_gain + norm_bias).astype(BF16)
    q = [normed[:, k * 448 : k * 448 + 448] for k in range(4)]
    q[0], q[1] = swap_if(core, q[0], q[1])
    q[2], q[3] = swap_if(core, q[2], q[3])
    near, far = jnp.concatenate(q[:2], 1), jnp.concatenate(q[2:], 1)
    near, far = swap_if(zl, near, far)

    column = jnp.concatenate([near] + [from_step(near, "x", k) for k in (1, 2, 3)], 0)
    near = jnp.concatenate([column] + [from_step(column, "y", k) for k in (1, 2, 3)], 0)
    column = jnp.concatenate([far] + [from_step(far, "y", k) for k in (1, 2, 3)], 0)
    far = [column] + [from_step(column, "x", k) for k in (1, 2, 3)]
    far = jnp.stack(far).reshape(4, 4, 40, 896).transpose(1, 0, 2, 3).reshape(640, 896)

    hidden = []
    for (even, odd), bias in zip(groups, biases):
        hidden.append(hidden_of(near, far, (*ring["in"][even], *ring["in"][odd]), bias))
    out = [None] * 4
    for block in (2, 3, 0, 1):
        w = [ring["out"][pair[block // 2]][block % 2] for pair in groups]
        out[block] = reduced(hidden, w, block % 2 == 0)
    out[0], out[2] = swap_if(zl, out[0], out[2])
    out[1], out[3] = swap_if(zl, out[1], out[3])
    out[0], out[1] = swap_if(core, out[0], out[1])
    out[2], out[3] = swap_if(core, out[2], out[3])
    return (values + jnp.concatenate(out, 1) + b_out).astype(BF16)


def solution(mesh):
    torus = Mesh(mesh.devices.reshape(2, 2, 4, 4, 4), AXES)
    return jax.shard_map(
        on_device,
        mesh=torus,
        in_specs=(P((*DP, *MP), None), P(), P(), P(DP, MP), P(MP), P(MP, DP), P()),
        out_specs=P((*DP, *MP), None),
        check_vma=False,
    )
```

```python
import jax
import jax.numpy as jnp
from jax import lax
from jax.experimental import pallas as pl
from jax.experimental.pallas import tpu as pltpu
from jax.sharding import Mesh
from jax.sharding import PartitionSpec as P

AXES = ("zl", "c", "x", "y", "zh")
MP = ("x", "y", "zh")
DP = ("zl", "c")
Z = ("zl", "zh")
PLANE = ("c", "x", "y")
F32, BF16 = jnp.float32, jnp.bfloat16


def z_index(z):
    return (z % 2) * 4 + (z % 8) // 2


def z_perm(k):
    pairs = []
    for z in range(8):
        source = z + k if z % 2 == 0 else z - k
        pairs.append((z_index(source), z_index(z)))
    return pairs


def towards(array):
    return lax.ppermute(array, Z, z_perm(1))


def away(array):
    return lax.ppermute(array, Z, z_perm(-1))


def other_core(array):
    return lax.ppermute(array, "c", [(0, 1), (1, 0)])


def plane_perm(stage, k):
    pairs = []
    for c in range(2):
        for x in range(4):
            for y in range(4):
                to = ((x + k) % 4, y) if (c + stage) % 2 == 0 else (x, (y + k) % 4)
                pairs.append((c * 16 + x * 4 + y, c * 16 + to[0] * 4 + to[1]))
    return pairs


def from_step(array, stage, k):
    return lax.ppermute(array, PLANE, plane_perm(stage, -k))


def to_step(array, stage, k):
    return lax.ppermute(array, PLANE, plane_perm(stage, k))


def gelu(value):
    return 0.5 * value * (1.0 + lax.erf(value * 0.7071067811865476))


def vmem():
    return pl.BlockSpec(memory_space=pltpu.VMEM)


LIMIT = pltpu.CompilerParams(vmem_limit_bytes=24 * 1024 * 1024)


def hidden_body(mine, theirs, own_even, own_odd, far_even, far_odd, bias_ref, out_ref, pre_ref):
    rows = mine.shape[1] // 2
    own = jnp.concatenate([own_even[:rows], own_odd[:rows]], 0)
    far = jnp.concatenate([far_even[:rows], far_odd[:rows]], 0)
    pre_ref[...] = jnp.dot(mine[...], own, preferred_element_type=F32) + jnp.dot(
        theirs[...], far, preferred_element_type=F32
    )
    three = bias_ref[rows : rows + 16, :].astype(F32)
    bias = three[0:1] + three[1:2] + three[2:3]
    step = 32

    @pl.loop(0, pre_ref.shape[0] // step)
    def _(i):
        at = pl.ds(pl.multiple_of(i * step, step), step)
        out_ref[at, :] = gelu(pre_ref[at, :] + bias).astype(BF16)


def hidden_of(mine, theirs, own_even, own_odd, far_even, far_odd):
    rows, cols = mine.shape[0], own_even.shape[1]
    return pl.pallas_call(
        hidden_body,
        out_shape=jax.ShapeDtypeStruct((rows, cols), BF16),
        in_specs=[vmem()] * 7,
        out_specs=vmem(),
        scratch_shapes=[pltpu.VMEM((rows, cols), F32)],
        compiler_params=LIMIT,
    )(mine, theirs, own_even, own_odd, far_even, far_odd, own_even)


def terms_body(*refs):
    own_h, far_h, even, odd = refs[:4], refs[4:8], refs[8:12], refs[12:16]
    pieces, sums = refs[16:20], refs[20]
    block = own_h[0].shape[0] // 16
    weights = [jnp.concatenate([e[...], o[...]], 0) for e, o in zip(even, odd)]
    for which, hidden in enumerate((own_h, far_h)):
        total = None
        for h, w in zip(hidden, weights):
            term = lax.dot_general(
                h[...], w, (((1,), (1,)), ((), ())), preferred_element_type=F32
            )
            total = term if total is None else total + term
        sums[...] = total
        for k, ref in enumerate(pieces):
            for m in range(4):
                at = (m * 4 + k if which == 0 else k * 4 + m) * block
                to = (2 * m + which) * block
                ref[to : to + block, :] = sums[at : at + block, :].astype(ref.dtype)


def terms_of(own_h, far_h, even, odd):
    rows, cols = own_h[0].shape[0], 2 * even[0].shape[0]
    shape = (rows // 2, cols)
    return pl.pallas_call(
        terms_body,
        out_shape=[jax.ShapeDtypeStruct(shape, F32)] + [jax.ShapeDtypeStruct(shape, BF16)] * 3,
        in_specs=[vmem()] * 16,
        out_specs=[vmem()] * 4,
        scratch_shapes=[pltpu.VMEM((rows, cols), F32)],
        compiler_params=LIMIT,
    )(*own_h, *far_h, *even, *odd)


def swap_if(flag, a, b):
    return jnp.where(flag, b, a), jnp.where(flag, a, b)


def three_parts(value):
    parts = []
    for _ in range(3):
        part = lax.reduce_precision(value, 8, 7)
        parts.append(part.astype(BF16))
        value = value - part
    return parts


def ring(own):
    got = {0: own, 1: towards(own), -1: away(own)}
    got[2], got[-2] = towards(got[-1]), away(got[1])
    got[3], got[-3] = towards(got[-2]), away(got[2])
    got[4] = towards(got[-3])
    return got


def on_device(tokens, norm_gain, norm_bias, w_in, b_in, w_out, b_out):
    zl, core = lax.axis_index("zl") == 1, lax.axis_index("c") == 1
    hold = tokens.shape[0]
    width = w_in.shape[0]
    bias = jnp.stack(three_parts(b_in))
    near_in = ring(jnp.concatenate([w_in, jnp.pad(bias, ((0, 13), (0, 0)))], 0))
    near_out = ring(w_out.T)
    far_in = {k: other_core(v) for k, v in near_in.items()}
    groups = ((0, 1), (-2, -1), (2, 3), (4, -3))

    values = tokens.astype(F32)
    center = jnp.mean(values, axis=1, keepdims=True)
    spread = jnp.mean((values - center) ** 2, axis=1, keepdims=True)
    normed = ((values - center) / jnp.sqrt(spread + 1e-06) * norm_gain + norm_bias).astype(BF16)
    q = [normed[:, k * width : k * width + width] for k in range(4)]
    q[0], q[2] = swap_if(zl, q[0], q[2])
    q[1], q[3] = swap_if(zl, q[1], q[3])
    q[0], q[1] = swap_if(core, q[0], q[1])
    q[2], q[3] = swap_if(core, q[2], q[3])
    both = jnp.concatenate(
        [jnp.concatenate([q[0], q[2]], 1), other_core(jnp.concatenate([q[1], q[3]], 1))], 0
    )
    row = jnp.concatenate([both] + [from_step(both, 0, k) for k in (1, 2, 3)], 0)
    plane = jnp.stack([row] + [from_step(row, 1, k) for k in (1, 2, 3)])
    plane = plane.reshape(4, 4, 2, hold, 2 * width)
    mine = plane[:, :, 0].reshape(16 * hold, 2 * width)
    theirs = other_core(plane[:, :, 1].transpose(1, 0, 2, 3).reshape(16 * hold, 2 * width))

    own_h = [
        hidden_of(mine, theirs, near_in[e], near_in[o], far_in[e], far_in[o]) for e, o in groups
    ]
    far_h = [other_core(h) for h in own_h]
    total, *sent = terms_of(
        own_h, far_h, [near_out[e] for e, _ in groups], [near_out[o] for _, o in groups]
    )
    for k, piece in enumerate(sent):
        total = total + to_step(piece, 0, k + 1).astype(F32)
    final = total[: 2 * hold]
    for k in (1, 2, 3):
        piece = total[2 * hold * k : 2 * hold * (k + 1)].astype(BF16)
        final = final + to_step(piece, 1, k).astype(F32)
    ours, others = final[:hold], other_core(final[hold:])
    out = [ours[:, :width], others[:, :width], ours[:, width:], others[:, width:]]
    out[0], out[1] = swap_if(core, out[0], out[1])
    out[2], out[3] = swap_if(core, out[2], out[3])
    out[0], out[2] = swap_if(zl, out[0], out[2])
    out[1], out[3] = swap_if(zl, out[1], out[3])
    return (values + jnp.concatenate(out, 1) + b_out).astype(BF16)


def solution(mesh):
    torus = Mesh(mesh.devices.reshape(2, 2, 4, 4, 4), AXES)
    return jax.shard_map(
        on_device,
        mesh=torus,
        in_specs=(P((*DP, *MP), None), P(), P(), P(DP, MP), P(MP), P(MP, DP), P()),
        out_specs=P((*DP, *MP), None),
        check_vma=False,
    )
```

```python
import jax
import jax.numpy as jnp
from jax import lax
from jax.experimental import pallas as pl
from jax.experimental.pallas import tpu as pltpu
from jax.sharding import Mesh
from jax.sharding import PartitionSpec as P

AXES = ("zl", "c", "x", "y", "zh")
MP = ("x", "y", "zh")
DP = ("zl", "c")
Z = ("zl", "zh")
PLANE = ("c", "x", "y")
F32, BF16 = jnp.float32, jnp.bfloat16


def z_index(z):
    return (z % 2) * 4 + (z % 8) // 2


def z_perm(k):
    pairs = []
    for z in range(8):
        source = z + k if z % 2 == 0 else z - k
        pairs.append((z_index(source), z_index(z)))
    return pairs


def towards(array):
    return lax.ppermute(array, Z, z_perm(1))


def away(array):
    return lax.ppermute(array, Z, z_perm(-1))


def other_core(array):
    return lax.ppermute(array, "c", [(0, 1), (1, 0)])


def plane_perm(stage, k):
    pairs = []
    for c in range(2):
        for x in range(4):
            for y in range(4):
                to = ((x + k) % 4, y) if (c + stage) % 2 == 0 else (x, (y + k) % 4)
                pairs.append((c * 16 + x * 4 + y, c * 16 + to[0] * 4 + to[1]))
    return pairs


def from_step(array, stage, k):
    return lax.ppermute(array, PLANE, plane_perm(stage, -k))


def to_step(array, stage, k):
    return lax.ppermute(array, PLANE, plane_perm(stage, k))


def gelu(value):
    return 0.5 * value * (1.0 + lax.erf(value * 0.7071067811865476))


def vmem():
    return pl.BlockSpec(memory_space=pltpu.VMEM)


LIMIT = pltpu.CompilerParams(vmem_limit_bytes=24 * 1024 * 1024)


def hidden_body(mine, theirs, own_even, own_odd, far_even, far_odd, bias_ref, out_ref, pre_ref):
    rows = mine.shape[1] // 2
    own = jnp.concatenate([own_even[...], own_odd[...]], 0)
    far = jnp.concatenate([far_even[...], far_odd[...]], 0)
    pre_ref[...] = jnp.dot(mine[...], own, preferred_element_type=F32) + jnp.dot(
        theirs[...], far, preferred_element_type=F32
    )
    three = bias_ref[rows : rows + 16, :].astype(F32)
    bias = three[0:1] + three[1:2] + three[2:3]
    step = 32

    @pl.loop(0, pre_ref.shape[0] // step)
    def _(i):
        at = pl.ds(pl.multiple_of(i * step, step), step)
        out_ref[at, :] = gelu(pre_ref[at, :] + bias).astype(BF16)


def hidden_of(mine, theirs, own_even, own_odd, far_even, far_odd, bias):
    rows, cols = mine.shape[0], own_even.shape[1]
    return pl.pallas_call(
        hidden_body,
        out_shape=jax.ShapeDtypeStruct((rows, cols), BF16),
        in_specs=[vmem()] * 7,
        out_specs=vmem(),
        scratch_shapes=[pltpu.VMEM((rows, cols), F32)],
        compiler_params=LIMIT,
    )(mine, theirs, own_even, own_odd, far_even, far_odd, bias)


def terms_body(*refs):
    own_h, far_h, weights = refs[:4], refs[4:8], refs[8:12]
    pieces, sums = refs[12:16], refs[16]
    block = own_h[0].shape[0] // 16
    for which, hidden in enumerate((own_h, far_h)):
        total = None
        for h, w in zip(hidden, weights):
            term = lax.dot_general(
                h[...], w[: sums.shape[1]], (((1,), (1,)), ((), ())), preferred_element_type=F32
            )
            total = term if total is None else total + term
        sums[...] = total
        for k, ref in enumerate(pieces):
            for m in range(4):
                at = (m * 4 + k if which == 0 else k * 4 + m) * block
                to = (2 * m + which) * block
                ref[to : to + block, :] = sums[at : at + block, :].astype(ref.dtype)


def terms_of(own_h, far_h, weights, width):
    rows = own_h[0].shape[0]
    shape = (rows // 2, width)
    return pl.pallas_call(
        terms_body,
        out_shape=[jax.ShapeDtypeStruct(shape, F32)] + [jax.ShapeDtypeStruct(shape, BF16)] * 3,
        in_specs=[vmem()] * 12,
        out_specs=[vmem()] * 4,
        scratch_shapes=[pltpu.VMEM((rows, width), F32)],
        compiler_params=LIMIT,
    )(*own_h, *far_h, *weights)


def row_body(*refs):
    pieces, out = refs[:-1], refs[-1]
    rows = pieces[0].shape[0]
    for k, piece in enumerate(pieces):
        out[k * rows : (k + 1) * rows, :] = piece[...]


def row_of(pieces):
    rows, cols = pieces[0].shape
    return pl.pallas_call(
        row_body,
        out_shape=jax.ShapeDtypeStruct((4 * rows, cols), BF16),
        in_specs=[vmem()] * 4,
        out_specs=vmem(),
        compiler_params=LIMIT,
    )(*pieces)


def plane_body(*refs):
    pieces, mine, theirs = refs[:4], refs[4], refs[5]
    block = pieces[0].shape[0] // 8
    for m, piece in enumerate(pieces):
        for k in range(4):
            at, a, b = 2 * k * block, (m * 4 + k) * block, (k * 4 + m) * block
            mine[a : a + block, :] = piece[at : at + block, :]
            theirs[b : b + block, :] = piece[at + block : at + 2 * block, :]


def plane_of(pieces):
    rows, cols = pieces[0].shape
    return pl.pallas_call(
        plane_body,
        out_shape=[jax.ShapeDtypeStruct((2 * rows, cols), BF16)] * 2,
        in_specs=[vmem()] * 4,
        out_specs=[vmem()] * 2,
        compiler_params=LIMIT,
    )(*pieces)


def swap_if(flag, a, b):
    return jnp.where(flag, b, a), jnp.where(flag, a, b)


def three_parts(value):
    parts = []
    for _ in range(3):
        part = lax.reduce_precision(value, 8, 7)
        parts.append(part.astype(BF16))
        value = value - part
    return parts


def ring(own, name):
    got = {0: own, 1: towards(own), -1: away(own)}
    for k in (2, 3):
        got[k] = towards(got[1 - k])
        got[-k] = away(got[k - 1])
    if name == "in":
        got[4] = towards(got[-3])
    else:
        got[4] = away(got[3])
    return got


def block(tokens, norm_gain, norm_bias, w_in, b_in, w_out, b_out):
    zl, core = lax.axis_index("zl") == 1, lax.axis_index("c") == 1
    hold = tokens.shape[0]
    width = w_in.shape[0]
    near_in = ring(w_in, "in")
    bias = jnp.pad(jnp.stack(three_parts(b_in)), ((0, 13), (0, 0)))
    near_out = ring(jnp.concatenate([w_out.T, bias], 0), "out")
    far_in = {k: other_core(v) for k, v in near_in.items()}
    groups = ((0, 1), (-2, -1), (2, 3), (4, -3))

    values = tokens.astype(F32)
    center = jnp.mean(values, axis=1, keepdims=True)
    spread = jnp.mean((values - center) ** 2, axis=1, keepdims=True)
    normed = ((values - center) / jnp.sqrt(spread + 1e-06) * norm_gain + norm_bias).astype(BF16)
    q = [normed[:, k * width : k * width + width] for k in range(4)]
    q[0], q[2] = swap_if(zl, q[0], q[2])
    q[1], q[3] = swap_if(zl, q[1], q[3])
    q[0], q[1] = swap_if(core, q[0], q[1])
    q[2], q[3] = swap_if(core, q[2], q[3])
    both = jnp.concatenate(
        [jnp.concatenate([q[0], q[2]], 1), other_core(jnp.concatenate([q[1], q[3]], 1))], 0
    )
    row = row_of([both] + [from_step(both, 0, k) for k in (1, 2, 3)])
    mine, theirs = plane_of([row] + [from_step(row, 1, k) for k in (1, 2, 3)])
    theirs = other_core(theirs)

    own_h = []
    for e, o in groups:
        bias = near_out[min(e, o, key=abs)]
        own_h.append(hidden_of(mine, theirs, near_in[e], near_in[o], far_in[e], far_in[o], bias))
    far_h = [other_core(h) for h in own_h]
    halves = []
    for which in (1, 0):
        weights = [near_out[pair[which]] for pair in groups]
        total, *sent = terms_of(own_h, far_h, weights, width)
        sent = [to_step(piece, 0, k + 1) for k, piece in enumerate(sent)]
        for piece in sent:
            total = total + piece.astype(F32)
        final = total[: 2 * hold]
        parts = [
            total[2 * hold * k : 2 * hold * (k + 1)].astype(BF16) for k in (1, 2, 3)
        ]
        for k, piece in enumerate(parts):
            final = final + to_step(piece, 1, k + 1).astype(F32)
        halves.append(final)
    final = jnp.concatenate(halves[::-1], 1)
    ours, others = final[:hold], other_core(final[hold:])
    out = [ours[:, :width], others[:, :width], ours[:, width:], others[:, width:]]
    out[0], out[1] = swap_if(core, out[0], out[1])
    out[2], out[3] = swap_if(core, out[2], out[3])
    out[0], out[2] = swap_if(zl, out[0], out[2])
    out[1], out[3] = swap_if(zl, out[1], out[3])
    return (values + jnp.concatenate(out, 1) + b_out).astype(BF16)


def solution(mesh):
    torus = Mesh(mesh.devices.reshape(2, 2, 4, 4, 4), AXES)
    return jax.shard_map(
        block,
        mesh=torus,
        in_specs=(P((*DP, *MP), None), P(), P(), P(DP, MP), P(MP), P(MP, DP), P()),
        out_specs=P((*DP, *MP), None),
        check_vma=False,
    )
```

```python
import jax
import jax.numpy as jnp
from jax import lax
from jax.experimental import pallas as pl
from jax.experimental.pallas import tpu as pltpu
from jax.sharding import Mesh
from jax.sharding import PartitionSpec as P

AXES = ("zl", "c", "x", "y", "zh")
MP = ("x", "y", "zh")
DP = ("zl", "c")
Z = ("zl", "zh")
PLANE = ("c", "x", "y")
F32, BF16 = jnp.float32, jnp.bfloat16


def z_index(z):
    return (z % 2) * 4 + (z % 8) // 2


def z_perm(k):
    pairs = []
    for z in range(8):
        source = z + k if z % 2 == 0 else z - k
        pairs.append((z_index(source), z_index(z)))
    return pairs


def towards(array):
    return lax.ppermute(array, Z, z_perm(1))


def away(array):
    return lax.ppermute(array, Z, z_perm(-1))


def other_core(array):
    return lax.ppermute(array, "c", [(0, 1), (1, 0)])


def plane_perm(stage, k):
    pairs = []
    for c in range(2):
        for x in range(4):
            for y in range(4):
                to = ((x + k) % 4, y) if (c + stage) % 2 == 0 else (x, (y + k) % 4)
                pairs.append((c * 16 + x * 4 + y, c * 16 + to[0] * 4 + to[1]))
    return pairs


def from_step(array, stage, k):
    return lax.ppermute(array, PLANE, plane_perm(stage, -k))


def to_step(array, stage, k):
    return lax.ppermute(array, PLANE, plane_perm(stage, k))


def gelu(value):
    return 0.5 * value * (1.0 + lax.erf(value * 0.7071067811865476))


def vmem():
    return pl.BlockSpec(memory_space=pltpu.VMEM)


LIMIT = pltpu.CompilerParams(vmem_limit_bytes=24 * 1024 * 1024)


def hidden_body(mine, theirs, own_even, own_odd, far_even, far_odd, bias_ref, out_ref, pre_ref):
    rows = mine.shape[1] // 2
    own = jnp.concatenate([own_even[...], own_odd[...]], 0)
    far = jnp.concatenate([far_even[...], far_odd[...]], 0)
    pre_ref[...] = jnp.dot(mine[...], own, preferred_element_type=F32) + jnp.dot(
        theirs[...], far, preferred_element_type=F32
    )
    three = bias_ref[rows : rows + 16, :].astype(F32)
    bias = three[0:1] + three[1:2] + three[2:3]
    step = 32

    @pl.loop(0, pre_ref.shape[0] // step)
    def _(i):
        at = pl.ds(pl.multiple_of(i * step, step), step)
        out_ref[at, :] = gelu(pre_ref[at, :] + bias).astype(BF16)


def hidden_of(mine, theirs, own_even, own_odd, far_even, far_odd, bias):
    rows, cols = mine.shape[0], own_even.shape[1]
    return pl.pallas_call(
        hidden_body,
        out_shape=jax.ShapeDtypeStruct((rows, cols), BF16),
        in_specs=[vmem()] * 7,
        out_specs=vmem(),
        scratch_shapes=[pltpu.VMEM((rows, cols), F32)],
        compiler_params=LIMIT,
    )(mine, theirs, own_even, own_odd, far_even, far_odd, bias)


def terms_body(*refs):
    own_h, far_h, weights = refs[:4], refs[4:8], refs[8:12]
    pieces, sums = refs[12:16], refs[16]
    block = own_h[0].shape[0] // 16
    for which, hidden in enumerate((own_h, far_h)):
        total = None
        for h, w in zip(hidden, weights):
            term = lax.dot_general(
                h[...], w[: sums.shape[1]], (((1,), (1,)), ((), ())), preferred_element_type=F32
            )
            total = term if total is None else total + term
        sums[...] = total
        for k, ref in enumerate(pieces):
            for m in range(4):
                at = (m * 4 + k if which == 0 else k * 4 + m) * block
                to = (2 * m + which) * block
                ref[to : to + block, :] = sums[at : at + block, :].astype(ref.dtype)


def terms_of(own_h, far_h, weights, width):
    rows = own_h[0].shape[0]
    shape = (rows // 2, width)
    return pl.pallas_call(
        terms_body,
        out_shape=[jax.ShapeDtypeStruct(shape, F32)] + [jax.ShapeDtypeStruct(shape, BF16)] * 3,
        in_specs=[vmem()] * 12,
        out_specs=[vmem()] * 4,
        scratch_shapes=[pltpu.VMEM((rows, width), F32)],
        compiler_params=LIMIT,
    )(*own_h, *far_h, *weights)


def norm_body(place, tokens, gain, bias, mine, theirs):
    values = tokens[...].astype(F32)
    center = jnp.mean(values, axis=1, keepdims=True)
    spread = jnp.mean((values - center) ** 2, axis=1, keepdims=True)
    normed = (values - center) / jnp.sqrt(spread + 1e-06) * gain[...] + bias[...]
    normed = normed.astype(BF16)
    width = mine.shape[1] // 2
    for zl in range(2):
        for c in range(2):

            @pl.when(place[0] == 2 * zl + c)
            def _():
                for half in range(2):
                    for ref, core in ((mine, c), (theirs, 1 - c)):
                        k = 2 * (zl ^ half) + core
                        ref[:, half * width : (half + 1) * width] = normed[
                            :, k * width : (k + 1) * width
                        ]


def norm_of(place, tokens, gain, bias):
    hold, features = tokens.shape
    return pl.pallas_call(
        norm_body,
        out_shape=[jax.ShapeDtypeStruct((hold, features // 2), BF16)] * 2,
        in_specs=[pl.BlockSpec(memory_space=pltpu.SMEM)] + [vmem()] * 3,
        out_specs=[vmem()] * 2,
        compiler_params=LIMIT,
    )(place, tokens, gain.reshape(1, -1), bias.reshape(1, -1))


def joined_body(weights, bias, out):
    rows, cols = weights.shape
    out[:rows, :] = weights[...]
    rest, at = bias[...], lax.broadcasted_iota(jnp.int32, (16, cols), 0)
    tail = jnp.zeros((16, cols), F32)
    for k in range(3):
        part = rest.astype(BF16).astype(F32)
        tail = jnp.where(at == k, part, tail)
        rest = rest - part
    out[rows : rows + 16, :] = tail.astype(BF16)


def joined_of(weights, bias):
    rows, cols = weights.shape
    return pl.pallas_call(
        joined_body,
        out_shape=jax.ShapeDtypeStruct((rows + 16, cols), BF16),
        in_specs=[vmem()] * 2,
        out_specs=vmem(),
        compiler_params=LIMIT,
    )(weights, bias.reshape(1, -1))


def row_body(*refs):
    pieces, out = refs[:-1], refs[-1]
    rows = pieces[0].shape[0]
    for k, piece in enumerate(pieces):
        out[k * rows : (k + 1) * rows, :] = piece[...]


def row_of(pieces):
    rows, cols = pieces[0].shape
    return pl.pallas_call(
        row_body,
        out_shape=jax.ShapeDtypeStruct((4 * rows, cols), BF16),
        in_specs=[vmem()] * 4,
        out_specs=vmem(),
        compiler_params=LIMIT,
    )(*pieces)


def plane_body(*refs):
    pieces, mine, theirs = refs[:4], refs[4], refs[5]
    block = pieces[0].shape[0] // 8
    for m, piece in enumerate(pieces):
        for k in range(4):
            at, a, b = 2 * k * block, (m * 4 + k) * block, (k * 4 + m) * block
            mine[a : a + block, :] = piece[at : at + block, :]
            theirs[b : b + block, :] = piece[at + block : at + 2 * block, :]


def plane_of(pieces):
    rows, cols = pieces[0].shape
    return pl.pallas_call(
        plane_body,
        out_shape=[jax.ShapeDtypeStruct((2 * rows, cols), BF16)] * 2,
        in_specs=[vmem()] * 4,
        out_specs=[vmem()] * 2,
        compiler_params=LIMIT,
    )(*pieces)


def sum_body(*refs):
    own, pieces = refs[8], refs[9:]
    rows = own.shape[0] // 2
    for half in range(2):
        total, *sent = refs[4 * half : 4 * half + 4]
        for k, out in enumerate((own, *pieces)):
            at = slice(k * rows, (k + 1) * rows)
            value = total[at, :]
            for piece in sent:
                value = value + piece[at, :].astype(F32)
            out[half * rows : (half + 1) * rows, :] = value.astype(out.dtype)


def sum_of(even, odd):
    rows, cols = even[0].shape
    shape = (rows // 2, cols)
    return pl.pallas_call(
        sum_body,
        out_shape=[jax.ShapeDtypeStruct(shape, F32)] + [jax.ShapeDtypeStruct(shape, BF16)] * 3,
        in_specs=[vmem()] * 8,
        out_specs=[vmem()] * 4,
        compiler_params=LIMIT,
    )(*even, *odd)


def last_body(own, s1, s2, s3, ours, others):
    hold = ours.shape[0] // 2
    for half in range(2):
        for k, out in enumerate((ours, others)):
            at = slice((2 * half + k) * hold, (2 * half + k + 1) * hold)
            value = own[at, :]
            for piece in (s1, s2, s3):
                value = value + piece[at, :].astype(F32)
            out[half * hold : (half + 1) * hold, :] = value


def last_of(own, sent):
    rows, cols = own.shape
    return pl.pallas_call(
        last_body,
        out_shape=[jax.ShapeDtypeStruct((rows // 2, cols), F32)] * 2,
        in_specs=[vmem()] * 4,
        out_specs=[vmem()] * 2,
        compiler_params=LIMIT,
    )(own, *sent)


def result_body(place, tokens, ours, others, bias, out):
    hold, width = tokens.shape[0], ours.shape[1]
    for zl in range(2):
        for c in range(2):

            @pl.when(place[0] == 2 * zl + c)
            def _():
                for half in range(2):
                    for ref, core in ((ours, c), (others, 1 - c)):
                        k = 2 * (zl ^ half) + core
                        at = slice(k * width, (k + 1) * width)
                        value = tokens[:, at].astype(F32) + ref[half * hold : (half + 1) * hold, :]
                        out[:, at] = (value + bias[:, at]).astype(BF16)


def result_of(place, tokens, ours, others, bias):
    return pl.pallas_call(
        result_body,
        out_shape=jax.ShapeDtypeStruct(tokens.shape, BF16),
        in_specs=[pl.BlockSpec(memory_space=pltpu.SMEM)] + [vmem()] * 4,
        out_specs=vmem(),
        compiler_params=LIMIT,
    )(place, tokens, ours, others, bias.reshape(1, -1))


def ring(own, name):
    got = {0: own, 1: towards(own), -1: away(own)}
    for k in (2, 3):
        got[k] = towards(got[1 - k])
        got[-k] = away(got[k - 1])
    if name == "in":
        got[4] = towards(got[-3])
    else:
        got[4] = away(got[3])
    return got


def block(tokens, norm_gain, norm_bias, w_in, b_in, w_out, b_out):
    width = w_in.shape[0]
    near_in = ring(w_in, "in")
    near_out = ring(joined_of(w_out.T, b_in), "out")
    far_in = {k: other_core(v) for k, v in near_in.items()}
    groups = ((0, 1), (-2, -1), (2, 3), (4, -3))

    place = (2 * lax.axis_index("zl") + lax.axis_index("c")).astype(jnp.int32).reshape(1)
    ours, others = norm_of(place, tokens, norm_gain, norm_bias)
    both = jnp.concatenate([ours, other_core(others)], 0)
    row = row_of([both] + [from_step(both, 0, k) for k in (1, 2, 3)])
    mine, theirs = plane_of([row] + [from_step(row, 1, k) for k in (1, 2, 3)])
    theirs = other_core(theirs)

    own_h = []
    for e, o in groups:
        bias = near_out[min(e, o, key=abs)]
        own_h.append(hidden_of(mine, theirs, near_in[e], near_in[o], far_in[e], far_in[o], bias))
    far_h = [other_core(h) for h in own_h]
    halves = []
    for which in (1, 0):
        weights = [near_out[pair[which]] for pair in groups]
        total, *sent = terms_of(own_h, far_h, weights, width)
        halves.append((total, *(to_step(piece, 0, k + 1) for k, piece in enumerate(sent))))
    own, *sent = sum_of(halves[1], halves[0])
    sent = [to_step(piece, 1, k + 1) for k, piece in enumerate(sent)]
    ours, others = last_of(own, sent)
    return result_of(place, tokens, ours, other_core(others), b_out)


def solution(mesh):
    torus = Mesh(mesh.devices.reshape(2, 2, 4, 4, 4), AXES)
    return jax.shard_map(
        block,
        mesh=torus,
        in_specs=(P((*DP, *MP), None), P(), P(), P(DP, MP), P(MP), P(MP, DP), P()),
        out_specs=P((*DP, *MP), None),
        check_vma=False,
    )
```

```python
import jax
import jax.numpy as jnp
from jax import lax
from jax.experimental import pallas as pl
from jax.experimental.pallas import tpu as pltpu
from jax.sharding import Mesh
from jax.sharding import PartitionSpec as P

AXES = ("zl", "c", "x", "y", "zh")
MP = ("x", "y", "zh")
DP = ("zl", "c")
Z = ("zl", "zh")
PLANE = ("c", "x", "y")
F32, BF16 = jnp.float32, jnp.bfloat16


def z_index(z):
    return (z % 2) * 4 + (z % 8) // 2


def z_perm(k):
    pairs = []
    for z in range(8):
        source = z + k if z % 2 == 0 else z - k
        pairs.append((z_index(source), z_index(z)))
    return pairs


def towards(array):
    return lax.ppermute(array, Z, z_perm(1))


def away(array):
    return lax.ppermute(array, Z, z_perm(-1))


def other_core(array):
    return lax.ppermute(array, "c", [(0, 1), (1, 0)])


def plane_perm(stage, k):
    pairs = []
    for c in range(2):
        for x in range(4):
            for y in range(4):
                to = ((x + k) % 4, y) if (c + stage) % 2 == 0 else (x, (y + k) % 4)
                pairs.append((c * 16 + x * 4 + y, c * 16 + to[0] * 4 + to[1]))
    return pairs


def from_step(array, stage, k):
    return lax.ppermute(array, PLANE, plane_perm(stage, -k))


def to_step(array, stage, k):
    return lax.ppermute(array, PLANE, plane_perm(stage, k))


def gelu(value):
    return 0.5 * value * (1.0 + lax.erf(value * 0.7071067811865476))


def vmem():
    return pl.BlockSpec(memory_space=pltpu.VMEM)


def in_hbm(array):
    return pltpu.with_memory_space_constraint(array, pltpu.HBM)


LIMIT = pltpu.CompilerParams(vmem_limit_bytes=24 * 1024 * 1024)


def hidden_body(mine, theirs, own_even, own_odd, far_even, far_odd, bias_ref, out_ref, pre_ref):
    rows = mine.shape[1] // 2
    own = jnp.concatenate([own_even[...], own_odd[...]], 0)
    far = jnp.concatenate([far_even[...], far_odd[...]], 0)
    pre_ref[...] = jnp.dot(mine[...], own, preferred_element_type=F32) + jnp.dot(
        theirs[...], far, preferred_element_type=F32
    )
    three = bias_ref[rows : rows + 16, :].astype(F32)
    bias = three[0:1] + three[1:2] + three[2:3]
    step = 32

    @pl.loop(0, pre_ref.shape[0] // step)
    def _(i):
        at = pl.ds(pl.multiple_of(i * step, step), step)
        out_ref[at, :] = gelu(pre_ref[at, :] + bias).astype(BF16)


def hidden_of(mine, theirs, own_even, own_odd, far_even, far_odd, bias):
    rows, cols = mine.shape[0], own_even.shape[1]
    return pl.pallas_call(
        hidden_body,
        out_shape=jax.ShapeDtypeStruct((rows, cols), BF16),
        in_specs=[vmem()] * 7,
        out_specs=vmem(),
        scratch_shapes=[pltpu.VMEM((rows, cols), F32)],
        compiler_params=LIMIT,
    )(mine, theirs, own_even, own_odd, far_even, far_odd, bias)


def terms_body(*refs):
    own_h, far_h, weights = refs[:4], refs[4:8], refs[8:12]
    pieces, sums = refs[12:16], refs[16]
    block = own_h[0].shape[0] // 16
    for which, hidden in enumerate((own_h, far_h)):
        total = None
        for h, w in zip(hidden, weights):
            term = lax.dot_general(
                h[...], w[: sums.shape[1]], (((1,), (1,)), ((), ())), preferred_element_type=F32
            )
            total = term if total is None else total + term
        sums[...] = total
        width = sums.shape[1]
        for k, ref in enumerate(pieces):
            for m in range(4):
                at = (m * 4 + k if which == 0 else k * 4 + m) * block
                ref[m * block : (m + 1) * block, which * width : (which + 1) * width] = sums[
                    at : at + block, :
                ].astype(ref.dtype)


def terms_of(own_h, far_h, weights, width):
    rows = own_h[0].shape[0]
    shape = (rows // 4, 2 * width)
    return pl.pallas_call(
        terms_body,
        out_shape=[jax.ShapeDtypeStruct(shape, F32)] + [jax.ShapeDtypeStruct(shape, BF16)] * 3,
        in_specs=[vmem()] * 12,
        out_specs=[vmem()] * 4,
        scratch_shapes=[pltpu.VMEM((rows, width), F32)],
        compiler_params=LIMIT,
    )(*own_h, *far_h, *weights)


def prologue_body(place, tokens, gain, bias, weights, b_in, mine, theirs, joined, *scratch):
    tok, gains, biases, b_ins, sems = scratch
    rows = weights.shape[0]
    copies = [
        pltpu.make_async_copy(source, target, sems.at[k])
        for k, (source, target) in enumerate(
            (
                (tokens, tok),
                (gain, gains),
                (bias, biases),
                (b_in, b_ins),
                (weights, joined.at[pl.ds(0, rows)]),
            )
        )
    ]
    for copy in copies:
        copy.start()
    copies[0].wait()
    values = tok[...].astype(F32)
    center = jnp.mean(values, axis=1, keepdims=True)
    spread = jnp.mean((values - center) ** 2, axis=1, keepdims=True)
    copies[1].wait()
    copies[2].wait()
    normed = (values - center) / jnp.sqrt(spread + 1e-06) * gains[...] + biases[...]
    normed = normed.astype(BF16)
    width = mine.shape[1] // 2
    for zl in range(2):
        for c in range(2):

            @pl.when(place[0] == 2 * zl + c)
            def _():
                for half in range(2):
                    for ref, core in ((mine, c), (theirs, 1 - c)):
                        k = 2 * (zl ^ half) + core
                        ref[:, half * width : (half + 1) * width] = normed[
                            :, k * width : (k + 1) * width
                        ]

    copies[3].wait()
    rest = b_ins[...]
    at = lax.broadcasted_iota(jnp.int32, (16, rest.shape[1]), 0)
    tail = jnp.zeros(at.shape, F32)
    for k in range(3):
        part = rest.astype(BF16).astype(F32)
        tail = jnp.where(at == k, part, tail)
        rest = rest - part
    joined[rows : rows + 16, :] = tail.astype(BF16)
    copies[4].wait()


def prologue_of(place, tokens, gain, bias, weights, b_in):
    hold, features = tokens.shape
    rows, cols = weights.shape
    row = (1, features)
    return pl.pallas_call(
        prologue_body,
        out_shape=[jax.ShapeDtypeStruct((hold, features // 2), BF16)] * 2
        + [jax.ShapeDtypeStruct((rows + 16, cols), BF16)],
        in_specs=[pl.BlockSpec(memory_space=pltpu.SMEM)]
        + [pl.BlockSpec(memory_space=pltpu.HBM)] * 5,
        out_specs=[vmem()] * 3,
        scratch_shapes=[
            pltpu.VMEM((hold, features), BF16),
            pltpu.VMEM(row, F32),
            pltpu.VMEM(row, F32),
            pltpu.VMEM((1, cols), F32),
            pltpu.SemaphoreType.DMA((5,)),
        ],
        compiler_params=LIMIT,
    )(place, *map(in_hbm, (tokens, gain.reshape(row), bias.reshape(row), weights, b_in.reshape(1, -1))))


def row_body(*refs):
    pieces, out = refs[:-1], refs[-1]
    rows = pieces[0].shape[0]
    for k, piece in enumerate(pieces):
        out[k * rows : (k + 1) * rows, :] = piece[...]


def row_of(pieces):
    rows, cols = pieces[0].shape
    return pl.pallas_call(
        row_body,
        out_shape=jax.ShapeDtypeStruct((4 * rows, cols), BF16),
        in_specs=[vmem()] * 4,
        out_specs=vmem(),
        compiler_params=LIMIT,
    )(*pieces)


def plane_body(*refs):
    pieces, mine, theirs = refs[:4], refs[4], refs[5]
    block = pieces[0].shape[0] // 8
    for m, piece in enumerate(pieces):
        for k in range(4):
            at, a, b = 2 * k * block, (m * 4 + k) * block, (k * 4 + m) * block
            mine[a : a + block, :] = piece[at : at + block, :]
            theirs[b : b + block, :] = piece[at + block : at + 2 * block, :]


def plane_of(pieces):
    rows, cols = pieces[0].shape
    return pl.pallas_call(
        plane_body,
        out_shape=[jax.ShapeDtypeStruct((2 * rows, cols), BF16)] * 2,
        in_specs=[vmem()] * 4,
        out_specs=[vmem()] * 2,
        compiler_params=LIMIT,
    )(*pieces)


def sum_body(*refs):
    own, pieces = refs[8], refs[9:]
    rows = own.shape[0] // 2
    for half in range(2):
        total, *sent = refs[4 * half : 4 * half + 4]
        for k, out in enumerate((own, *pieces)):
            at = slice(k * rows, (k + 1) * rows)
            value = total[at, :]
            for piece in sent:
                value = value + piece[at, :].astype(F32)
            out[half * rows : (half + 1) * rows, :] = value.astype(out.dtype)


def sum_of(even, odd):
    rows, cols = even[0].shape
    shape = (rows // 2, cols)
    return pl.pallas_call(
        sum_body,
        out_shape=[jax.ShapeDtypeStruct(shape, F32)] + [jax.ShapeDtypeStruct(shape, BF16)] * 3,
        in_specs=[vmem()] * 8,
        out_specs=[vmem()] * 4,
        compiler_params=LIMIT,
    )(*even, *odd)


def last_body(own, s1, s2, s3, ours, others):
    value = own[...]
    for piece in (s1, s2, s3):
        value = value + piece[...].astype(F32)
    width = ours.shape[1]
    ours[...] = value[:, :width]
    others[...] = value[:, width:]


def last_of(own, sent):
    rows, cols = own.shape
    return pl.pallas_call(
        last_body,
        out_shape=[jax.ShapeDtypeStruct((rows, cols // 2), F32)] * 2,
        in_specs=[vmem()] * 4,
        out_specs=[vmem()] * 2,
        compiler_params=LIMIT,
    )(own, *sent)


def result_body(place, tokens, ours, others, bias, out):
    hold, width = tokens.shape[0], ours.shape[1]
    for zl in range(2):
        for c in range(2):

            @pl.when(place[0] == 2 * zl + c)
            def _():
                for half in range(2):
                    for ref, core in ((ours, c), (others, 1 - c)):
                        k = 2 * (zl ^ half) + core
                        at = slice(k * width, (k + 1) * width)
                        value = tokens[:, at].astype(F32) + ref[half * hold : (half + 1) * hold, :]
                        out[:, at] = (value + bias[:, at]).astype(BF16)


def result_of(place, tokens, ours, others, bias):
    return pl.pallas_call(
        result_body,
        out_shape=jax.ShapeDtypeStruct(tokens.shape, BF16),
        in_specs=[pl.BlockSpec(memory_space=pltpu.SMEM)] + [vmem()] * 4,
        out_specs=vmem(),
        compiler_params=LIMIT,
    )(place, tokens, ours, others, bias.reshape(1, -1))


def ring(own, name):
    got = {0: own, 1: towards(own), -1: away(own)}
    for k in (2, 3):
        got[k] = towards(got[1 - k])
        got[-k] = away(got[k - 1])
    if name == "in":
        got[4] = towards(got[-3])
    else:
        got[4] = away(got[3])
    return got


def block(tokens, norm_gain, norm_bias, w_in, b_in, w_out, b_out):
    width = w_in.shape[0]
    near_in = ring(w_in, "in")
    place = (2 * lax.axis_index("zl") + lax.axis_index("c")).astype(jnp.int32).reshape(1)
    ours, others, joined = prologue_of(place, tokens, norm_gain, norm_bias, w_out.T, b_in)
    near_out = ring(joined, "out")
    far_in = {k: other_core(v) for k, v in near_in.items()}
    groups = ((0, 1), (-2, -1), (2, 3), (4, -3))

    both = jnp.concatenate([ours, other_core(others)], 0)
    row = row_of([both] + [from_step(both, 0, k) for k in (1, 2, 3)])
    mine, theirs = plane_of([row] + [from_step(row, 1, k) for k in (1, 2, 3)])
    theirs = other_core(theirs)

    own_h = []
    for e, o in groups:
        bias = near_out[min(e, o, key=abs)]
        own_h.append(hidden_of(mine, theirs, near_in[e], near_in[o], far_in[e], far_in[o], bias))
    far_h = [other_core(h) for h in own_h]
    halves = []
    for which in (1, 0):
        weights = [near_out[pair[which]] for pair in groups]
        total, *sent = terms_of(own_h, far_h, weights, width)
        halves.append((total, *(to_step(piece, 0, k + 1) for k, piece in enumerate(sent))))
    own, *sent = sum_of(halves[1], halves[0])
    sent = [to_step(piece, 1, k + 1) for k, piece in enumerate(sent)]
    ours, others = last_of(own, sent)
    return result_of(place, tokens, ours, other_core(others), b_out)


def solution(mesh):
    torus = Mesh(mesh.devices.reshape(2, 2, 4, 4, 4), AXES)
    return jax.shard_map(
        block,
        mesh=torus,
        in_specs=(P((*DP, *MP), None), P(), P(), P(DP, MP), P(MP), P(MP, DP), P()),
        out_specs=P((*DP, *MP), None),
        check_vma=False,
    )
```

```python
import functools

import jax
import jax.numpy as jnp
from jax import lax
from jax.experimental import pallas as pl
from jax.experimental.pallas import tpu as pltpu
from jax.sharding import Mesh
from jax.sharding import PartitionSpec as P

AXES = ("zl", "c", "x", "y", "zh")
MP = ("x", "y", "zh")
DP = ("zl", "c")
Z = ("zl", "zh")
PLANE = ("c", "x", "y")
F32, BF16 = jnp.float32, jnp.bfloat16


def z_index(z):
    return (z % 2) * 4 + (z % 8) // 2


def z_perm(k):
    pairs = []
    for z in range(8):
        source = z + k if z % 2 == 0 else z - k
        pairs.append((z_index(source), z_index(z)))
    return pairs


def towards(array):
    return lax.ppermute(array, Z, z_perm(1))


def away(array):
    return lax.ppermute(array, Z, z_perm(-1))


def other_core(array):
    return lax.ppermute(array, "c", [(0, 1), (1, 0)])


def plane_perm(stage, k):
    pairs = []
    for c in range(2):
        for x in range(4):
            for y in range(4):
                to = ((x + k) % 4, y) if (c + stage) % 2 == 0 else (x, (y + k) % 4)
                pairs.append((c * 16 + x * 4 + y, c * 16 + to[0] * 4 + to[1]))
    return pairs


def from_step(array, stage, k):
    return lax.ppermute(array, PLANE, plane_perm(stage, -k))


def to_step(array, stage, k):
    return lax.ppermute(array, PLANE, plane_perm(stage, k))


def gelu(value):
    return 0.5 * value * (1.0 + lax.erf(value * 0.7071067811865476))


def row_of_tiles(tiles):
    return jnp.concatenate([tiles[k : k + 1, :] for k in range(tiles.shape[0])], 1)


def vmem():
    return pl.BlockSpec(memory_space=pltpu.VMEM)


def in_hbm(array):
    return pltpu.with_memory_space_constraint(array, pltpu.HBM)


LIMIT = pltpu.CompilerParams(vmem_limit_bytes=24 * 1024 * 1024)


def hidden_body(mine, theirs, own_even, own_odd, far_even, far_odd, bias_ref, out_ref, pre_ref):
    rows = mine.shape[1] // 2
    own = jnp.concatenate([own_even[...], own_odd[...]], 0)
    far = jnp.concatenate([far_even[...], far_odd[...]], 0)
    pre_ref[...] = jnp.dot(mine[...], own, preferred_element_type=F32) + jnp.dot(
        theirs[...], far, preferred_element_type=F32
    )
    three = bias_ref[rows : rows + 16, :].astype(F32)
    bias = three[0:1] + three[1:2] + three[2:3]
    step = 32

    @pl.loop(0, pre_ref.shape[0] // step)
    def _(i):
        at = pl.ds(pl.multiple_of(i * step, step), step)
        out_ref[at, :] = gelu(pre_ref[at, :] + bias).astype(BF16)


def hidden_of(mine, theirs, own_even, own_odd, far_even, far_odd, bias):
    rows, cols = mine.shape[0], own_even.shape[1]
    return pl.pallas_call(
        hidden_body,
        out_shape=jax.ShapeDtypeStruct((rows, cols), BF16),
        in_specs=[vmem()] * 7,
        out_specs=vmem(),
        scratch_shapes=[pltpu.VMEM((rows, cols), F32)],
        compiler_params=LIMIT,
    )(mine, theirs, own_even, own_odd, far_even, far_odd, bias)


def term_of(hidden, weights, width):
    total = None
    for h, w in zip(hidden, weights):
        term = lax.dot_general(
            h[...], w[:width], (((1,), (1,)), ((), ())), preferred_element_type=F32
        )
        total = term if total is None else total + term
    return total


def part_body(*refs):
    groups, out = (len(refs) - 1) // 3, refs[-1]
    weights = refs[2 * groups : 3 * groups]
    rows = refs[0].shape[0]
    for which in range(2):
        hidden = refs[which * groups : (which + 1) * groups]
        out[which * rows : (which + 1) * rows, :] = term_of(hidden, weights, out.shape[1])


def part_of(own_h, far_h, weights, width):
    return pl.pallas_call(
        part_body,
        out_shape=jax.ShapeDtypeStruct((2 * own_h[0].shape[0], width), F32),
        in_specs=[vmem()] * (3 * len(own_h)),
        out_specs=vmem(),
        compiler_params=LIMIT,
    )(*own_h, *far_h, *weights)


def terms_body(groups, *refs):
    weights, before = refs[2 * groups : 3 * groups], refs[3 * groups : -5]
    pieces, sums = refs[-5:-1], refs[-1]
    rows, width = sums.shape
    block = rows // 16
    for which in range(2):
        total = term_of(refs[which * groups : (which + 1) * groups], weights, width)
        for part in before:
            total = total + part[which * rows : (which + 1) * rows, :]
        sums[...] = total
        for k, ref in enumerate(pieces):
            for m in range(4):
                at = (m * 4 + k if which == 0 else k * 4 + m) * block
                ref[m * block : (m + 1) * block, which * width : (which + 1) * width] = sums[
                    at : at + block, :
                ].astype(ref.dtype)


def terms_of(own_h, far_h, weights, width, *before):
    rows, groups = own_h[0].shape[0], len(own_h)
    shape = (rows // 4, 2 * width)
    return pl.pallas_call(
        functools.partial(terms_body, groups),
        out_shape=[jax.ShapeDtypeStruct(shape, F32)] + [jax.ShapeDtypeStruct(shape, BF16)] * 3,
        in_specs=[vmem()] * (3 * groups + len(before)),
        out_specs=[vmem()] * 4,
        scratch_shapes=[pltpu.VMEM((rows, width), F32)],
        compiler_params=LIMIT,
    )(*own_h, *far_h, *weights, *before)


def prologue_body(place, tokens, gain, bias, weights, b_in, mine, theirs, joined, *scratch):
    tok, gains, biases, b_ins, sems = scratch
    rows = weights.shape[0]
    copies = [
        pltpu.make_async_copy(source, target, sems.at[k])
        for k, (source, target) in enumerate(
            (
                (tokens, tok),
                (gain, gains),
                (bias, biases),
                (b_in, b_ins),
                (weights, joined.at[pl.ds(0, rows)]),
            )
        )
    ]
    for copy in copies:
        copy.start()
    copies[0].wait()
    values = tok[...].astype(F32)
    center = jnp.mean(values, axis=1, keepdims=True)
    spread = jnp.mean((values - center) ** 2, axis=1, keepdims=True)
    copies[1].wait()
    copies[2].wait()
    normed = (values - center) / jnp.sqrt(spread + 1e-06) * row_of_tiles(gains[...]) + row_of_tiles(biases[...])
    normed = normed.astype(BF16)
    width = mine.shape[1] // 2
    for zl in range(2):
        for c in range(2):

            @pl.when(place[0] == 2 * zl + c)
            def _():
                for half in range(2):
                    for ref, core in ((mine, c), (theirs, 1 - c)):
                        k = 2 * (zl ^ half) + core
                        ref[:, half * width : (half + 1) * width] = normed[
                            :, k * width : (k + 1) * width
                        ]

    copies[3].wait()
    rest = b_ins[...]
    at = lax.broadcasted_iota(jnp.int32, (16, rest.shape[1]), 0)
    tail = jnp.zeros(at.shape, F32)
    for k in range(3):
        part = rest.astype(BF16).astype(F32)
        tail = jnp.where(at == k, part, tail)
        rest = rest - part
    joined[rows : rows + 16, :] = tail.astype(BF16)
    copies[4].wait()


def prologue_of(place, tokens, gain, bias, weights, b_in):
    hold, features = tokens.shape
    rows, cols = weights.shape
    row = (features // 128, 128)
    return pl.pallas_call(
        prologue_body,
        out_shape=[jax.ShapeDtypeStruct((hold, features // 2), BF16)] * 2
        + [jax.ShapeDtypeStruct((rows + 16, cols), BF16)],
        in_specs=[pl.BlockSpec(memory_space=pltpu.SMEM)]
        + [pl.BlockSpec(memory_space=pltpu.HBM)] * 5,
        out_specs=[vmem()] * 3,
        scratch_shapes=[
            pltpu.VMEM((hold, features), BF16),
            pltpu.VMEM(row, F32),
            pltpu.VMEM(row, F32),
            pltpu.VMEM((1, cols), F32),
            pltpu.SemaphoreType.DMA((5,)),
        ],
        compiler_params=LIMIT,
    )(place, *map(in_hbm, (tokens, gain.reshape(row), bias.reshape(row), weights, b_in.reshape(1, -1))))


def row_body(*refs):
    pieces, out = refs[:-1], refs[-1]
    rows = pieces[0].shape[0]
    for k, piece in enumerate(pieces):
        out[k * rows : (k + 1) * rows, :] = piece[...]


def row_of(pieces):
    rows, cols = pieces[0].shape
    return pl.pallas_call(
        row_body,
        out_shape=jax.ShapeDtypeStruct((4 * rows, cols), BF16),
        in_specs=[vmem()] * 4,
        out_specs=vmem(),
        compiler_params=LIMIT,
    )(*pieces)


def plane_body(*refs):
    pieces, mine, theirs = refs[:4], refs[4], refs[5]
    block = pieces[0].shape[0] // 8
    for m, piece in enumerate(pieces):
        for k in range(4):
            at, a, b = 2 * k * block, (m * 4 + k) * block, (k * 4 + m) * block
            mine[a : a + block, :] = piece[at : at + block, :]
            theirs[b : b + block, :] = piece[at + block : at + 2 * block, :]


def plane_of(pieces):
    rows, cols = pieces[0].shape
    return pl.pallas_call(
        plane_body,
        out_shape=[jax.ShapeDtypeStruct((2 * rows, cols), BF16)] * 2,
        in_specs=[vmem()] * 4,
        out_specs=[vmem()] * 2,
        compiler_params=LIMIT,
    )(*pieces)


def sum_body(*refs):
    own, pieces = refs[8], refs[9:]
    rows = own.shape[0] // 2
    for half in range(2):
        total, *sent = refs[4 * half : 4 * half + 4]
        for k, out in enumerate((own, *pieces)):
            at = slice(k * rows, (k + 1) * rows)
            value = total[at, :]
            for piece in sent:
                value = value + piece[at, :].astype(F32)
            out[half * rows : (half + 1) * rows, :] = value.astype(out.dtype)


def sum_of(even, odd):
    rows, cols = even[0].shape
    shape = (rows // 2, cols)
    return pl.pallas_call(
        sum_body,
        out_shape=[jax.ShapeDtypeStruct(shape, F32)] + [jax.ShapeDtypeStruct(shape, BF16)] * 3,
        in_specs=[vmem()] * 8,
        out_specs=[vmem()] * 4,
        compiler_params=LIMIT,
    )(*even, *odd)


def last_body(own, s1, s2, s3, ours, others):
    value = own[...]
    for piece in (s1, s2, s3):
        value = value + piece[...].astype(F32)
    width = ours.shape[1]
    ours[...] = value[:, :width]
    others[...] = value[:, width:]


def last_of(own, sent):
    rows, cols = own.shape
    return pl.pallas_call(
        last_body,
        out_shape=[jax.ShapeDtypeStruct((rows, cols // 2), F32)] * 2,
        in_specs=[vmem()] * 4,
        out_specs=[vmem()] * 2,
        compiler_params=LIMIT,
    )(own, *sent)


def result_body(place, tokens, ours, others, bias, out):
    hold, width = tokens.shape[0], ours.shape[1]
    biases = row_of_tiles(bias[...])
    for zl in range(2):
        for c in range(2):

            @pl.when(place[0] == 2 * zl + c)
            def _():
                for half in range(2):
                    for ref, core in ((ours, c), (others, 1 - c)):
                        k = 2 * (zl ^ half) + core
                        at = slice(k * width, (k + 1) * width)
                        value = tokens[:, at].astype(F32) + ref[half * hold : (half + 1) * hold, :]
                        out[:, at] = (value + biases[:, at]).astype(BF16)


def result_of(place, tokens, ours, others, bias):
    return pl.pallas_call(
        result_body,
        out_shape=jax.ShapeDtypeStruct(tokens.shape, BF16),
        in_specs=[pl.BlockSpec(memory_space=pltpu.SMEM)] + [vmem()] * 4,
        out_specs=vmem(),
        compiler_params=LIMIT,
    )(place, tokens, ours, others, bias.reshape(-1, 128))


def ring(own, name):
    got = {0: own, 1: towards(own), -1: away(own)}
    for k in (2, 3):
        got[k] = towards(got[1 - k])
        got[-k] = away(got[k - 1])
    if name == "in":
        got[4] = towards(got[-3])
    else:
        got[4] = away(got[3])
    return got


def block(tokens, norm_gain, norm_bias, w_in, b_in, w_out, b_out):
    width = w_in.shape[0]
    near_in = ring(w_in, "in")
    place = (2 * lax.axis_index("zl") + lax.axis_index("c")).astype(jnp.int32).reshape(1)
    ours, others, joined = prologue_of(place, tokens, norm_gain, norm_bias, w_out.T, b_in)
    near_out = ring(joined, "out")
    far_in = {k: other_core(v) for k, v in near_in.items()}
    groups = ((0, 1), (-2, -1), (2, 3), (4, -3))

    both = jnp.concatenate([ours, other_core(others)], 0)
    row = row_of([both] + [from_step(both, 0, k) for k in (1, 2, 3)])
    mine, theirs = plane_of([row] + [from_step(row, 1, k) for k in (1, 2, 3)])
    theirs = other_core(theirs)

    own_h = []
    for e, o in groups:
        bias = near_out[min(e, o, key=abs)]
        own_h.append(hidden_of(mine, theirs, near_in[e], near_in[o], far_in[e], far_in[o], bias))
    far_h = [other_core(h) for h in own_h]
    halves = []
    for which, name in ((1, "odd"), (0, "even")):
        weights = [near_out[pair[which]] for pair in groups]
        if name == "odd":
            part = part_of(own_h[:3], far_h[:3], weights[:3], width)
            total, *sent = terms_of(own_h[3:], far_h[3:], weights[3:], width, part)
        else:
            total, *sent = terms_of(own_h, far_h, weights, width)
        halves.append((total, *(to_step(piece, 0, k + 1) for k, piece in enumerate(sent))))
    own, *sent = sum_of(halves[1], halves[0])
    sent = [to_step(piece, 1, k + 1) for k, piece in enumerate(sent)]
    ours, others = last_of(own, sent)
    return result_of(place, tokens, ours, other_core(others), b_out)


def solution(mesh):
    torus = Mesh(mesh.devices.reshape(2, 2, 4, 4, 4), AXES)
    return jax.shard_map(
        block,
        mesh=torus,
        in_specs=(P((*DP, *MP), None), P(), P(), P(DP, MP), P(MP), P(MP, DP), P()),
        out_specs=P((*DP, *MP), None),
        check_vma=False,
    )
```

```python
import functools

import jax
import jax.numpy as jnp
from jax import lax
from jax.experimental import pallas as pl
from jax.experimental.pallas import tpu as pltpu
from jax.sharding import Mesh
from jax.sharding import PartitionSpec as P

AXES = ("zl", "c", "x", "y", "zh")
MP = ("x", "y", "zh")
DP = ("zl", "c")
Z = ("zl", "zh")
PLANE = ("c", "x", "y")
F32, BF16 = jnp.float32, jnp.bfloat16


def z_index(z):
    return (z % 2) * 4 + (z % 8) // 2


def z_perm(k):
    pairs = []
    for z in range(8):
        source = z + k if z % 2 == 0 else z - k
        pairs.append((z_index(source), z_index(z)))
    return pairs


def towards(array):
    return lax.ppermute(array, Z, z_perm(1))


def away(array):
    return lax.ppermute(array, Z, z_perm(-1))


def other_core(array):
    return lax.ppermute(array, "c", [(0, 1), (1, 0)])


def plane_perm(stage, k):
    pairs = []
    for c in range(2):
        for x in range(4):
            for y in range(4):
                to = ((x + k) % 4, y) if (c + stage) % 2 == 0 else (x, (y + k) % 4)
                pairs.append((c * 16 + x * 4 + y, c * 16 + to[0] * 4 + to[1]))
    return pairs


def from_step(array, stage, k):
    return lax.ppermute(array, PLANE, plane_perm(stage, -k))


def to_step(array, stage, k):
    return lax.ppermute(array, PLANE, plane_perm(stage, k))


def gelu(value):
    return 0.5 * value * (1.0 + lax.erf(value * 0.7071067811865476))


def row_of_tiles(tiles):
    return jnp.concatenate([tiles[k : k + 1, :] for k in range(tiles.shape[0])], 1)


def vmem():
    return pl.BlockSpec(memory_space=pltpu.VMEM)


def in_hbm(array):
    return pltpu.with_memory_space_constraint(array, pltpu.HBM)


LIMIT = pltpu.CompilerParams(vmem_limit_bytes=24 * 1024 * 1024)


def hidden_body(mine, theirs, own_even, own_odd, far_even, far_odd, bias_ref, out_ref):
    rows = mine.shape[1] // 2
    own = jnp.concatenate([own_even[...], own_odd[...]], 0)
    far = jnp.concatenate([far_even[...], far_odd[...]], 0)
    three = bias_ref[rows : rows + 16, :].astype(F32)
    bias = three[0:1] + three[1:2] + three[2:3]
    step = out_ref.shape[0] // 2
    for i in range(2):
        at = slice(i * step, (i + 1) * step)
        pre = jnp.dot(mine[at, :], own, preferred_element_type=F32) + jnp.dot(
            theirs[at, :], far, preferred_element_type=F32
        )
        out_ref[at, :] = gelu(pre + bias).astype(BF16)


def hidden_of(mine, theirs, own_even, own_odd, far_even, far_odd, bias):
    rows, cols = mine.shape[0], own_even.shape[1]
    return pl.pallas_call(
        hidden_body,
        out_shape=jax.ShapeDtypeStruct((rows, cols), BF16),
        in_specs=[vmem()] * 7,
        out_specs=vmem(),
        compiler_params=LIMIT,
    )(mine, theirs, own_even, own_odd, far_even, far_odd, bias)


def term_of(hidden, weights, width):
    total = None
    for h, w in zip(hidden, weights):
        term = lax.dot_general(
            h[...], w[:width], (((1,), (1,)), ((), ())), preferred_element_type=F32
        )
        total = term if total is None else total + term
    return total


def part_body(*refs):
    groups, out = (len(refs) - 1) // 3, refs[-1]
    weights = refs[2 * groups : 3 * groups]
    rows = refs[0].shape[0]
    for which in range(2):
        hidden = refs[which * groups : (which + 1) * groups]
        out[which * rows : (which + 1) * rows, :] = term_of(hidden, weights, out.shape[1])


def part_of(own_h, far_h, weights, width):
    return pl.pallas_call(
        part_body,
        out_shape=jax.ShapeDtypeStruct((2 * own_h[0].shape[0], width), F32),
        in_specs=[vmem()] * (3 * len(own_h)),
        out_specs=vmem(),
        compiler_params=LIMIT,
    )(*own_h, *far_h, *weights)


def terms_body(groups, *refs):
    weights, before = refs[2 * groups : 3 * groups], refs[3 * groups : -5]
    pieces, sums = refs[-5:-1], refs[-1]
    rows, width = sums.shape
    block = rows // 16
    for which in range(2):
        total = term_of(refs[which * groups : (which + 1) * groups], weights, width)
        for part in before:
            total = total + part[which * rows : (which + 1) * rows, :]
        sums[...] = total
        for k, ref in enumerate(pieces):
            for m in range(4):
                at = (m * 4 + k if which == 0 else k * 4 + m) * block
                ref[m * block : (m + 1) * block, which * width : (which + 1) * width] = sums[
                    at : at + block, :
                ].astype(ref.dtype)


def terms_of(own_h, far_h, weights, width, *before):
    rows, groups = own_h[0].shape[0], len(own_h)
    shape = (rows // 4, 2 * width)
    return pl.pallas_call(
        functools.partial(terms_body, groups),
        out_shape=[jax.ShapeDtypeStruct(shape, F32)] + [jax.ShapeDtypeStruct(shape, BF16)] * 3,
        in_specs=[vmem()] * (3 * groups + len(before)),
        out_specs=[vmem()] * 4,
        scratch_shapes=[pltpu.VMEM((rows, width), F32)],
        compiler_params=LIMIT,
    )(*own_h, *far_h, *weights, *before)


def prologue_body(place, tokens, gain, bias, weights, b_in, mine, theirs, joined, *scratch):
    tok, gains, biases, b_ins, sems = scratch
    rows = weights.shape[0]
    copies = [
        pltpu.make_async_copy(source, target, sems.at[k])
        for k, (source, target) in enumerate(
            (
                (tokens, tok),
                (gain, gains),
                (bias, biases),
                (b_in, b_ins),
                (weights, joined.at[pl.ds(0, rows)]),
            )
        )
    ]
    for copy in copies:
        copy.start()
    copies[0].wait()
    values = tok[...].astype(F32)
    center = jnp.mean(values, axis=1, keepdims=True)
    spread = jnp.mean((values - center) ** 2, axis=1, keepdims=True)
    copies[1].wait()
    copies[2].wait()
    normed = (values - center) / jnp.sqrt(spread + 1e-06) * row_of_tiles(gains[...]) + row_of_tiles(biases[...])
    normed = normed.astype(BF16)
    width = mine.shape[1] // 2
    for zl in range(2):
        for c in range(2):

            @pl.when(place[0] == 2 * zl + c)
            def _():
                for half in range(2):
                    for ref, core in ((mine, c), (theirs, 1 - c)):
                        k = 2 * (zl ^ half) + core
                        ref[:, half * width : (half + 1) * width] = normed[
                            :, k * width : (k + 1) * width
                        ]

    copies[3].wait()
    rest = b_ins[...]
    at = lax.broadcasted_iota(jnp.int32, (16, rest.shape[1]), 0)
    tail = jnp.zeros(at.shape, F32)
    for k in range(3):
        part = rest.astype(BF16).astype(F32)
        tail = jnp.where(at == k, part, tail)
        rest = rest - part
    joined[rows : rows + 16, :] = tail.astype(BF16)
    copies[4].wait()


def prologue_of(place, tokens, gain, bias, weights, b_in):
    hold, features = tokens.shape
    rows, cols = weights.shape
    row = (features // 128, 128)
    return pl.pallas_call(
        prologue_body,
        out_shape=[jax.ShapeDtypeStruct((hold, features // 2), BF16)] * 2
        + [jax.ShapeDtypeStruct((rows + 16, cols), BF16)],
        in_specs=[pl.BlockSpec(memory_space=pltpu.SMEM)]
        + [pl.BlockSpec(memory_space=pltpu.HBM)] * 5,
        out_specs=[vmem()] * 3,
        scratch_shapes=[
            pltpu.VMEM((hold, features), BF16),
            pltpu.VMEM(row, F32),
            pltpu.VMEM(row, F32),
            pltpu.VMEM((1, cols), F32),
            pltpu.SemaphoreType.DMA((5,)),
        ],
        compiler_params=LIMIT,
    )(place, *map(in_hbm, (tokens, gain.reshape(row), bias.reshape(row), weights, b_in.reshape(1, -1))))


def row_body(*refs):
    pieces, out = refs[:-1], refs[-1]
    rows = pieces[0].shape[0]
    for k, piece in enumerate(pieces):
        out[k * rows : (k + 1) * rows, :] = piece[...]


def row_of(pieces):
    rows, cols = pieces[0].shape
    return pl.pallas_call(
        row_body,
        out_shape=jax.ShapeDtypeStruct((4 * rows, cols), BF16),
        in_specs=[vmem()] * 4,
        out_specs=vmem(),
        compiler_params=LIMIT,
    )(*pieces)


def plane_body(*refs):
    pieces, mine, theirs = refs[:4], refs[4], refs[5]
    block = pieces[0].shape[0] // 8
    for m, piece in enumerate(pieces):
        for k in range(4):
            at, a, b = 2 * k * block, (m * 4 + k) * block, (k * 4 + m) * block
            mine[a : a + block, :] = piece[at : at + block, :]
            theirs[b : b + block, :] = piece[at + block : at + 2 * block, :]


def plane_of(pieces):
    rows, cols = pieces[0].shape
    return pl.pallas_call(
        plane_body,
        out_shape=[jax.ShapeDtypeStruct((2 * rows, cols), BF16)] * 2,
        in_specs=[vmem()] * 4,
        out_specs=[vmem()] * 2,
        compiler_params=LIMIT,
    )(*pieces)


def sum_body(*refs):
    own, pieces = refs[8], refs[9:]
    rows = own.shape[0] // 2
    for half in range(2):
        total, *sent = refs[4 * half : 4 * half + 4]
        for k, out in enumerate((own, *pieces)):
            at = slice(k * rows, (k + 1) * rows)
            value = total[at, :]
            for piece in sent:
                value = value + piece[at, :].astype(F32)
            out[half * rows : (half + 1) * rows, :] = value.astype(out.dtype)


def sum_of(even, odd):
    rows, cols = even[0].shape
    shape = (rows // 2, cols)
    return pl.pallas_call(
        sum_body,
        out_shape=[jax.ShapeDtypeStruct(shape, F32)] + [jax.ShapeDtypeStruct(shape, BF16)] * 3,
        in_specs=[vmem()] * 8,
        out_specs=[vmem()] * 4,
        compiler_params=LIMIT,
    )(*even, *odd)


def last_body(own, s1, s2, s3, ours, others):
    value = own[...]
    for piece in (s1, s2, s3):
        value = value + piece[...].astype(F32)
    width = ours.shape[1]
    ours[...] = value[:, :width]
    others[...] = value[:, width:]


def last_of(own, sent):
    rows, cols = own.shape
    return pl.pallas_call(
        last_body,
        out_shape=[jax.ShapeDtypeStruct((rows, cols // 2), F32)] * 2,
        in_specs=[vmem()] * 4,
        out_specs=[vmem()] * 2,
        compiler_params=LIMIT,
    )(own, *sent)


def result_body(place, tokens, ours, others, bias, out):
    hold, width = tokens.shape[0], ours.shape[1]
    biases = row_of_tiles(bias[...])
    for zl in range(2):
        for c in range(2):

            @pl.when(place[0] == 2 * zl + c)
            def _():
                for half in range(2):
                    for ref, core in ((ours, c), (others, 1 - c)):
                        k = 2 * (zl ^ half) + core
                        at = slice(k * width, (k + 1) * width)
                        value = tokens[:, at].astype(F32) + ref[half * hold : (half + 1) * hold, :]
                        out[:, at] = (value + biases[:, at]).astype(BF16)


def result_of(place, tokens, ours, others, bias):
    return pl.pallas_call(
        result_body,
        out_shape=jax.ShapeDtypeStruct(tokens.shape, BF16),
        in_specs=[pl.BlockSpec(memory_space=pltpu.SMEM)] + [vmem()] * 4,
        out_specs=vmem(),
        compiler_params=LIMIT,
    )(place, tokens, ours, others, bias.reshape(-1, 128))


def ring(own, name):
    got = {0: own, 1: towards(own), -1: away(own)}
    for k in (2, 3):
        got[k] = towards(got[1 - k])
        got[-k] = away(got[k - 1])
    if name == "in":
        got[4] = towards(got[-3])
    else:
        got[4] = away(got[3])
    return got


def block(tokens, norm_gain, norm_bias, w_in, b_in, w_out, b_out):
    width = w_in.shape[0]
    near_in = ring(w_in, "in")
    place = (2 * lax.axis_index("zl") + lax.axis_index("c")).astype(jnp.int32).reshape(1)
    ours, others, joined = prologue_of(place, tokens, norm_gain, norm_bias, w_out.T, b_in)
    near_out = ring(joined, "out")
    far_in = {k: other_core(v) for k, v in near_in.items()}
    groups = ((0, 1), (-2, -1), (2, 3), (4, -3))

    both = jnp.concatenate([ours, other_core(others)], 0)
    row = row_of([both] + [from_step(both, 0, k) for k in (1, 2, 3)])
    mine, theirs = plane_of([row] + [from_step(row, 1, k) for k in (1, 2, 3)])
    theirs = other_core(theirs)

    own_h = []
    for e, o in groups:
        bias = near_out[min(e, o, key=abs)]
        own_h.append(hidden_of(mine, theirs, near_in[e], near_in[o], far_in[e], far_in[o], bias))
    far_h = [other_core(h) for h in own_h]
    halves = []
    for which, name in ((1, "odd"), (0, "even")):
        weights = [near_out[pair[which]] for pair in groups]
        if name == "odd":
            part = part_of(own_h[:3], far_h[:3], weights[:3], width)
            total, *sent = terms_of(own_h[3:], far_h[3:], weights[3:], width, part)
        else:
            total, *sent = terms_of(own_h, far_h, weights, width)
        halves.append((total, *(to_step(piece, 0, k + 1) for k, piece in enumerate(sent))))
    own, *sent = sum_of(halves[1], halves[0])
    sent = [to_step(piece, 1, k + 1) for k, piece in enumerate(sent)]
    ours, others = last_of(own, sent)
    return result_of(place, tokens, ours, other_core(others), b_out)


def solution(mesh):
    torus = Mesh(mesh.devices.reshape(2, 2, 4, 4, 4), AXES)
    return jax.shard_map(
        block,
        mesh=torus,
        in_specs=(P((*DP, *MP), None), P(), P(), P(DP, MP), P(MP), P(MP, DP), P()),
        out_specs=P((*DP, *MP), None),
        check_vma=False,
    )
```

```python
import functools

import jax
import jax.numpy as jnp
from jax import lax
from jax.experimental import pallas as pl
from jax.experimental.pallas import tpu as pltpu
from jax.sharding import Mesh
from jax.sharding import PartitionSpec as P

AXES = ("zl", "c", "x", "y", "zh")
MP = ("x", "y", "zh")
DP = ("zl", "c")
Z = ("zl", "zh")
PLANE = ("c", "x", "y")
F32, BF16 = jnp.float32, jnp.bfloat16


def z_index(z):
    return (z % 2) * 4 + (z % 8) // 2


def z_perm(k):
    pairs = []
    for z in range(8):
        source = z + k if z % 2 == 0 else z - k
        pairs.append((z_index(source), z_index(z)))
    return pairs


def towards(array):
    return lax.ppermute(array, Z, z_perm(1))


def away(array):
    return lax.ppermute(array, Z, z_perm(-1))


def other_core(array):
    return lax.ppermute(array, "c", [(0, 1), (1, 0)])


def plane_perm(stage, k):
    pairs = []
    for c in range(2):
        for x in range(4):
            for y in range(4):
                to = ((x + k) % 4, y) if (c + stage) % 2 == 0 else (x, (y + k) % 4)
                pairs.append((c * 16 + x * 4 + y, c * 16 + to[0] * 4 + to[1]))
    return pairs


def from_step(array, stage, k):
    return lax.ppermute(array, PLANE, plane_perm(stage, -k))


def to_step(array, stage, k):
    return lax.ppermute(array, PLANE, plane_perm(stage, k))


def gelu(value):
    return 0.5 * value * (1.0 + lax.erf(value * 0.7071067811865476))


def row_of_tiles(tiles):
    return jnp.concatenate([tiles[k : k + 1, :] for k in range(tiles.shape[0])], 1)


def vmem():
    return pl.BlockSpec(memory_space=pltpu.VMEM)


def in_hbm(array):
    return pltpu.with_memory_space_constraint(array, pltpu.HBM)


LIMIT = pltpu.CompilerParams(vmem_limit_bytes=24 * 1024 * 1024)


def hidden_body(mine, theirs, own_even, own_odd, far_even, far_odd, bias_ref, out_ref):
    rows = mine.shape[1] // 2
    own = jnp.concatenate([own_even[...], own_odd[...]], 0)
    far = jnp.concatenate([far_even[...], far_odd[...]], 0)
    three = bias_ref[rows : rows + 16, :].astype(F32)
    bias = three[0:1] + three[1:2] + three[2:3]
    step = out_ref.shape[0] // 2
    for i in range(2):
        at = slice(i * step, (i + 1) * step)
        pre = jnp.dot(mine[at, :], own, preferred_element_type=F32) + jnp.dot(
            theirs[at, :], far, preferred_element_type=F32
        )
        out_ref[at, :] = gelu(pre + bias).astype(BF16)


def hidden_of(mine, theirs, own_even, own_odd, far_even, far_odd, bias):
    rows, cols = mine.shape[0], own_even.shape[1]
    return pl.pallas_call(
        hidden_body,
        out_shape=jax.ShapeDtypeStruct((rows, cols), BF16),
        in_specs=[vmem()] * 7,
        out_specs=vmem(),
        compiler_params=LIMIT,
    )(mine, theirs, own_even, own_odd, far_even, far_odd, bias)


def term_of(hidden, weights, width):
    total = None
    for h, w in zip(hidden, weights):
        term = lax.dot_general(
            h[...], w[:width], (((1,), (1,)), ((), ())), preferred_element_type=F32
        )
        total = term if total is None else total + term
    return total


def part_body(*refs):
    groups, out = (len(refs) - 1) // 3, refs[-1]
    weights = refs[2 * groups : 3 * groups]
    rows = refs[0].shape[0]
    for which in range(2):
        hidden = refs[which * groups : (which + 1) * groups]
        out[which * rows : (which + 1) * rows, :] = term_of(hidden, weights, out.shape[1])


def part_of(own_h, far_h, weights, width):
    return pl.pallas_call(
        part_body,
        out_shape=jax.ShapeDtypeStruct((2 * own_h[0].shape[0], width), F32),
        in_specs=[vmem()] * (3 * len(own_h)),
        out_specs=vmem(),
        compiler_params=LIMIT,
    )(*own_h, *far_h, *weights)


def terms_body(groups, stage, *refs):
    weights, before = refs[2 * groups : 3 * groups], refs[3 * groups : -5]
    pieces, sums = refs[-5:-1], refs[-1]
    rows, width = sums.shape
    block = rows // 16
    for which in range(2):
        total = term_of(refs[which * groups : (which + 1) * groups], weights, width)
        for part in before:
            total = total + part[which * rows : (which + 1) * rows, :]
        sums[...] = total
        for k, ref in enumerate(pieces):
            for m in range(4):
                at = (m * 4 + k if which == stage else k * 4 + m) * block
                ref[m * block : (m + 1) * block, which * width : (which + 1) * width] = sums[
                    at : at + block, :
                ].astype(ref.dtype)


def terms_of(own_h, far_h, weights, width, stage, *before):
    rows, groups = own_h[0].shape[0], len(own_h)
    shape = (rows // 4, 2 * width)
    return pl.pallas_call(
        functools.partial(terms_body, groups, stage),
        out_shape=[jax.ShapeDtypeStruct(shape, F32)] + [jax.ShapeDtypeStruct(shape, BF16)] * 3,
        in_specs=[vmem()] * (3 * groups + len(before)),
        out_specs=[vmem()] * 4,
        scratch_shapes=[pltpu.VMEM((rows, width), F32)],
        compiler_params=LIMIT,
    )(*own_h, *far_h, *weights, *before)


def prologue_body(place, tokens, gain, bias, weights, b_in, mine, theirs, joined, *scratch):
    tok, gains, biases, b_ins, sems = scratch
    rows = weights.shape[0]
    copies = [
        pltpu.make_async_copy(source, target, sems.at[k])
        for k, (source, target) in enumerate(
            (
                (tokens, tok),
                (gain, gains),
                (bias, biases),
                (b_in, b_ins),
                (weights, joined.at[pl.ds(0, rows)]),
            )
        )
    ]
    for copy in copies:
        copy.start()
    copies[0].wait()
    values = tok[...].astype(F32)
    center = jnp.mean(values, axis=1, keepdims=True)
    spread = jnp.mean((values - center) ** 2, axis=1, keepdims=True)
    copies[1].wait()
    copies[2].wait()
    normed = (values - center) / jnp.sqrt(spread + 1e-06) * row_of_tiles(gains[...]) + row_of_tiles(biases[...])
    normed = normed.astype(BF16)
    width = mine.shape[1] // 2
    for zl in range(2):
        for c in range(2):

            @pl.when(place[0] == 2 * zl + c)
            def _():
                for half in range(2):
                    for ref, core in ((mine, c), (theirs, 1 - c)):
                        k = 2 * (zl ^ half) + core
                        ref[:, half * width : (half + 1) * width] = normed[
                            :, k * width : (k + 1) * width
                        ]

    copies[3].wait()
    rest = b_ins[...]
    at = lax.broadcasted_iota(jnp.int32, (16, rest.shape[1]), 0)
    tail = jnp.zeros(at.shape, F32)
    for k in range(3):
        part = rest.astype(BF16).astype(F32)
        tail = jnp.where(at == k, part, tail)
        rest = rest - part
    joined[rows : rows + 16, :] = tail.astype(BF16)
    copies[4].wait()


def prologue_of(place, tokens, gain, bias, weights, b_in):
    hold, features = tokens.shape
    rows, cols = weights.shape
    row = (features // 128, 128)
    return pl.pallas_call(
        prologue_body,
        out_shape=[jax.ShapeDtypeStruct((hold, features // 2), BF16)] * 2
        + [jax.ShapeDtypeStruct((rows + 16, cols), BF16)],
        in_specs=[pl.BlockSpec(memory_space=pltpu.SMEM)]
        + [pl.BlockSpec(memory_space=pltpu.HBM)] * 5,
        out_specs=[vmem()] * 3,
        scratch_shapes=[
            pltpu.VMEM((hold, features), BF16),
            pltpu.VMEM(row, F32),
            pltpu.VMEM(row, F32),
            pltpu.VMEM((1, cols), F32),
            pltpu.SemaphoreType.DMA((5,)),
        ],
        compiler_params=LIMIT,
    )(place, *map(in_hbm, (tokens, gain.reshape(row), bias.reshape(row), weights, b_in.reshape(1, -1))))


def row_body(*refs):
    pieces, out = refs[:-1], refs[-1]
    rows = pieces[0].shape[0]
    for k, piece in enumerate(pieces):
        out[k * rows : (k + 1) * rows, :] = piece[...]


def row_of(pieces):
    rows, cols = pieces[0].shape
    return pl.pallas_call(
        row_body,
        out_shape=jax.ShapeDtypeStruct((4 * rows, cols), BF16),
        in_specs=[vmem()] * 4,
        out_specs=vmem(),
        compiler_params=LIMIT,
    )(*pieces)


def plane_body(*refs):
    pieces, mine, theirs = refs[:4], refs[4], refs[5]
    block = pieces[0].shape[0] // 8
    for m, piece in enumerate(pieces):
        for k in range(4):
            at, a, b = 2 * k * block, (m * 4 + k) * block, (k * 4 + m) * block
            mine[a : a + block, :] = piece[at : at + block, :]
            theirs[b : b + block, :] = piece[at + block : at + 2 * block, :]


def plane_of(pieces):
    rows, cols = pieces[0].shape
    return pl.pallas_call(
        plane_body,
        out_shape=[jax.ShapeDtypeStruct((2 * rows, cols), BF16)] * 2,
        in_specs=[vmem()] * 4,
        out_specs=[vmem()] * 2,
        compiler_params=LIMIT,
    )(*pieces)


def sum_body(total, s1, s2, s3, *pieces):
    rows = pieces[0].shape[0]
    for k, out in enumerate(pieces):
        at = slice(k * rows, (k + 1) * rows)
        value = total[at, :]
        for piece in (s1, s2, s3):
            value = value + piece[at, :].astype(F32)
        out[...] = value.astype(out.dtype)


def sum_of(total, sent):
    rows, cols = total.shape
    shape = (rows // 4, cols)
    return pl.pallas_call(
        sum_body,
        out_shape=[jax.ShapeDtypeStruct(shape, F32)] + [jax.ShapeDtypeStruct(shape, BF16)] * 3,
        in_specs=[vmem()] * 4,
        out_specs=[vmem()] * 4,
        compiler_params=LIMIT,
    )(total, *sent)


def last_body(*refs):
    ours, others = refs[-2:]
    rows, width = ours.shape[0] // 2, ours.shape[1]
    for half in range(2):
        own, *sent = refs[4 * half : 4 * half + 4]
        value = own[...]
        for piece in sent:
            value = value + piece[...].astype(F32)
        at = slice(half * rows, (half + 1) * rows)
        ours[at, :] = value[:, :width]
        others[at, :] = value[:, width:]


def last_of(even, odd):
    rows, cols = even[0].shape
    return pl.pallas_call(
        last_body,
        out_shape=[jax.ShapeDtypeStruct((2 * rows, cols // 2), F32)] * 2,
        in_specs=[vmem()] * 8,
        out_specs=[vmem()] * 2,
        compiler_params=LIMIT,
    )(*even, *odd)


def result_body(place, tokens, ours, others, bias, out):
    hold, width = tokens.shape[0], ours.shape[1]
    biases = row_of_tiles(bias[...])
    for zl in range(2):
        for c in range(2):

            @pl.when(place[0] == 2 * zl + c)
            def _():
                for half in range(2):
                    for ref, core in ((ours, c), (others, 1 - c)):
                        k = 2 * (zl ^ half) + core
                        at = slice(k * width, (k + 1) * width)
                        value = tokens[:, at].astype(F32) + ref[half * hold : (half + 1) * hold, :]
                        out[:, at] = (value + biases[:, at]).astype(BF16)


def result_of(place, tokens, ours, others, bias):
    return pl.pallas_call(
        result_body,
        out_shape=jax.ShapeDtypeStruct(tokens.shape, BF16),
        in_specs=[pl.BlockSpec(memory_space=pltpu.SMEM)] + [vmem()] * 4,
        out_specs=vmem(),
        compiler_params=LIMIT,
    )(place, tokens, ours, others, bias.reshape(-1, 128))


def ring(own, name):
    got = {0: own, 1: towards(own), -1: away(own)}
    for k in (2, 3):
        got[k] = towards(got[1 - k])
        got[-k] = away(got[k - 1])
    if name == "in":
        got[4] = towards(got[-3])
    else:
        got[4] = away(got[3])
    return got


def block(tokens, norm_gain, norm_bias, w_in, b_in, w_out, b_out):
    width = w_in.shape[0]
    near_in = ring(w_in, "in")
    place = (2 * lax.axis_index("zl") + lax.axis_index("c")).astype(jnp.int32).reshape(1)
    ours, others, joined = prologue_of(place, tokens, norm_gain, norm_bias, w_out.T, b_in)
    near_out = ring(joined, "out")
    far_in = {k: other_core(v) for k, v in near_in.items()}
    groups = ((0, 1), (-2, -1), (2, 3), (4, -3))

    both = jnp.concatenate([ours, other_core(others)], 0)
    row = row_of([both] + [from_step(both, 0, k) for k in (1, 2, 3)])
    mine, theirs = plane_of([row] + [from_step(row, 1, k) for k in (1, 2, 3)])
    theirs = other_core(theirs)

    own_h = []
    for e, o in groups:
        bias = near_out[min(e, o, key=abs)]
        own_h.append(hidden_of(mine, theirs, near_in[e], near_in[o], far_in[e], far_in[o], bias))
    far_h = [other_core(h) for h in own_h]
    halves = [None] * 2
    for which, stage in ((1, 0), (0, 1)):
        weights = [near_out[pair[which]] for pair in groups]
        part = part_of(own_h[:3], far_h[:3], weights[:3], width)
        total, *sent = terms_of(own_h[3:], far_h[3:], weights[3:], width, stage, part)
        sent = [to_step(piece, stage, k + 1) for k, piece in enumerate(sent)]
        own, *sent = sum_of(total, sent)
        sent = [to_step(piece, 1 - stage, k + 1) for k, piece in enumerate(sent)]
        halves[which] = (own, *sent)
    ours, others = last_of(*halves)
    return result_of(place, tokens, ours, other_core(others), b_out)


def solution(mesh):
    torus = Mesh(mesh.devices.reshape(2, 2, 4, 4, 4), AXES)
    return jax.shard_map(
        block,
        mesh=torus,
        in_specs=(P((*DP, *MP), None), P(), P(), P(DP, MP), P(MP), P(MP, DP), P()),
        out_specs=P((*DP, *MP), None),
        check_vma=False,
    )
```

```python
import functools

import jax
import jax.numpy as jnp
from jax import lax
from jax.experimental import pallas as pl
from jax.experimental.pallas import tpu as pltpu
from jax.sharding import Mesh
from jax.sharding import PartitionSpec as P

AXES = ("zl", "c", "x", "y", "zh")
MP = ("x", "y", "zh")
DP = ("zl", "c")
Z = ("zl", "zh")
PLANE = ("c", "x", "y")
F32, BF16 = jnp.float32, jnp.bfloat16


def z_index(z):
    return (z % 2) * 4 + (z % 8) // 2


def z_perm(k):
    pairs = []
    for z in range(8):
        source = z + k if z % 2 == 0 else z - k
        pairs.append((z_index(source), z_index(z)))
    return pairs


def towards(array):
    return lax.ppermute(array, Z, z_perm(1))


def away(array):
    return lax.ppermute(array, Z, z_perm(-1))


def other_core(array):
    return lax.ppermute(array, "c", [(0, 1), (1, 0)])


def plane_perm(stage, k):
    pairs = []
    for c in range(2):
        for x in range(4):
            for y in range(4):
                to = ((x + k) % 4, y) if (c + stage) % 2 == 0 else (x, (y + k) % 4)
                pairs.append((c * 16 + x * 4 + y, c * 16 + to[0] * 4 + to[1]))
    return pairs


def from_step(array, stage, k):
    return lax.ppermute(array, PLANE, plane_perm(stage, -k))


def to_step(array, stage, k):
    return lax.ppermute(array, PLANE, plane_perm(stage, k))


def gelu(value):
    return 0.5 * value * (1.0 + lax.erf(value * 0.7071067811865476))


def row_of_tiles(tiles):
    return jnp.concatenate([tiles[k : k + 1, :] for k in range(tiles.shape[0])], 1)


def vmem():
    return pl.BlockSpec(memory_space=pltpu.VMEM)


def in_hbm(array):
    return pltpu.with_memory_space_constraint(array, pltpu.HBM)


LIMIT = pltpu.CompilerParams(vmem_limit_bytes=24 * 1024 * 1024)


def pre_body(mine, own_even, own_odd, out_ref):
    own = jnp.concatenate([own_even[...], own_odd[...]], 0)
    out_ref[...] = jnp.dot(mine[...], own, preferred_element_type=F32)


def pre_of(mine, own_even, own_odd):
    return pl.pallas_call(
        pre_body,
        out_shape=jax.ShapeDtypeStruct((mine.shape[0], own_even.shape[1]), F32),
        in_specs=[vmem()] * 3,
        out_specs=vmem(),
        compiler_params=LIMIT,
    )(mine, own_even, own_odd)


def hidden_body(theirs, far_even, far_odd, bias_ref, *refs):
    before, out_ref = refs[:-1], refs[-1]
    rows = theirs.shape[1] // 2
    far = jnp.concatenate([far_even[...], far_odd[...]], 0)
    three = bias_ref[rows : rows + 16, :].astype(F32)
    bias = three[0:1] + three[1:2] + three[2:3]
    if len(before) == 3:
        own = jnp.concatenate([before[1][...], before[2][...]], 0)
    step = out_ref.shape[0] // 4
    for i in range(4):
        at = slice(i * step, (i + 1) * step)
        pre = jnp.dot(theirs[at, :], far, preferred_element_type=F32)
        if len(before) == 3:
            pre = jnp.dot(before[0][at, :], own, preferred_element_type=F32) + pre
        else:
            pre = before[0][at, :] + pre
        out_ref[at, :] = gelu(pre + bias).astype(BF16)


def hidden_of(theirs, far_even, far_odd, bias, *before):
    rows, cols = theirs.shape[0], far_even.shape[1]
    return pl.pallas_call(
        hidden_body,
        out_shape=jax.ShapeDtypeStruct((rows, cols), BF16),
        in_specs=[vmem()] * (4 + len(before)),
        out_specs=vmem(),
        compiler_params=LIMIT,
    )(theirs, far_even, far_odd, bias, *before)


def term_of(hidden, weights, width):
    total = None
    for h, w in zip(hidden, weights):
        term = lax.dot_general(
            h[...], w[:width], (((1,), (1,)), ((), ())), preferred_element_type=F32
        )
        total = term if total is None else total + term
    return total


def part_body(*refs):
    groups, out = (len(refs) - 1) // 3, refs[-1]
    weights = refs[2 * groups : 3 * groups]
    rows = refs[0].shape[0]
    for which in range(2):
        hidden = refs[which * groups : (which + 1) * groups]
        out[which * rows : (which + 1) * rows, :] = term_of(hidden, weights, out.shape[1])


def part_of(own_h, far_h, weights, width):
    return pl.pallas_call(
        part_body,
        out_shape=jax.ShapeDtypeStruct((2 * own_h[0].shape[0], width), F32),
        in_specs=[vmem()] * (3 * len(own_h)),
        out_specs=vmem(),
        compiler_params=LIMIT,
    )(*own_h, *far_h, *weights)


def terms_body(groups, stage, *refs):
    weights, before = refs[2 * groups : 3 * groups], refs[3 * groups : -5]
    pieces, sums = refs[-5:-1], refs[-1]
    rows, width = sums.shape
    block = rows // 16
    for which in range(2):
        total = term_of(refs[which * groups : (which + 1) * groups], weights, width)
        for part in before:
            total = total + part[which * rows : (which + 1) * rows, :]
        sums[...] = total
        for k, ref in enumerate(pieces):
            for m in range(4):
                at = (m * 4 + k if which == stage else k * 4 + m) * block
                ref[m * block : (m + 1) * block, which * width : (which + 1) * width] = sums[
                    at : at + block, :
                ].astype(ref.dtype)


def terms_of(own_h, far_h, weights, width, stage, *before):
    rows, groups = own_h[0].shape[0], len(own_h)
    shape = (rows // 4, 2 * width)
    return pl.pallas_call(
        functools.partial(terms_body, groups, stage),
        out_shape=[jax.ShapeDtypeStruct(shape, F32)] + [jax.ShapeDtypeStruct(shape, BF16)] * 3,
        in_specs=[vmem()] * (3 * groups + len(before)),
        out_specs=[vmem()] * 4,
        scratch_shapes=[pltpu.VMEM((rows, width), F32)],
        compiler_params=LIMIT,
    )(*own_h, *far_h, *weights, *before)


def prologue_body(place, tokens, gain, bias, weights, b_in, mine, theirs, joined, *scratch):
    tok, gains, biases, b_ins, sems = scratch
    rows = weights.shape[0]
    copies = [
        pltpu.make_async_copy(source, target, sems.at[k])
        for k, (source, target) in enumerate(
            (
                (tokens, tok),
                (gain, gains),
                (bias, biases),
                (b_in, b_ins),
                (weights, joined.at[pl.ds(0, rows)]),
            )
        )
    ]
    for copy in copies:
        copy.start()
    copies[0].wait()
    values = tok[...].astype(F32)
    center = jnp.mean(values, axis=1, keepdims=True)
    spread = jnp.mean((values - center) ** 2, axis=1, keepdims=True)
    copies[1].wait()
    copies[2].wait()
    normed = (values - center) / jnp.sqrt(spread + 1e-06) * row_of_tiles(gains[...]) + row_of_tiles(biases[...])
    normed = normed.astype(BF16)
    width = mine.shape[1] // 2
    for zl in range(2):
        for c in range(2):

            @pl.when(place[0] == 2 * zl + c)
            def _():
                for half in range(2):
                    for ref, core in ((mine, c), (theirs, 1 - c)):
                        k = 2 * (zl ^ half) + core
                        ref[:, half * width : (half + 1) * width] = normed[
                            :, k * width : (k + 1) * width
                        ]

    copies[3].wait()
    rest = b_ins[...]
    at = lax.broadcasted_iota(jnp.int32, (16, rest.shape[1]), 0)
    tail = jnp.zeros(at.shape, F32)
    for k in range(3):
        part = rest.astype(BF16).astype(F32)
        tail = jnp.where(at == k, part, tail)
        rest = rest - part
    joined[rows : rows + 16, :] = tail.astype(BF16)
    copies[4].wait()


def prologue_of(place, tokens, gain, bias, weights, b_in):
    hold, features = tokens.shape
    rows, cols = weights.shape
    row = (features // 128, 128)
    return pl.pallas_call(
        prologue_body,
        out_shape=[jax.ShapeDtypeStruct((hold, features // 2), BF16)] * 2
        + [jax.ShapeDtypeStruct((rows + 16, cols), BF16)],
        in_specs=[pl.BlockSpec(memory_space=pltpu.SMEM)]
        + [pl.BlockSpec(memory_space=pltpu.HBM)] * 5,
        out_specs=[vmem()] * 3,
        scratch_shapes=[
            pltpu.VMEM((hold, features), BF16),
            pltpu.VMEM(row, F32),
            pltpu.VMEM(row, F32),
            pltpu.VMEM((1, cols), F32),
            pltpu.SemaphoreType.DMA((5,)),
        ],
        compiler_params=LIMIT,
    )(place, *map(in_hbm, (tokens, gain.reshape(row), bias.reshape(row), weights, b_in.reshape(1, -1))))


def row_body(*refs):
    pieces, out = refs[:-1], refs[-1]
    rows = pieces[0].shape[0]
    for k, piece in enumerate(pieces):
        out[k * rows : (k + 1) * rows, :] = piece[...]


def row_of(pieces):
    rows, cols = pieces[0].shape
    return pl.pallas_call(
        row_body,
        out_shape=jax.ShapeDtypeStruct((4 * rows, cols), BF16),
        in_specs=[vmem()] * 4,
        out_specs=vmem(),
        compiler_params=LIMIT,
    )(*pieces)


def plane_body(*refs):
    pieces, mine, theirs = refs[:4], refs[4], refs[5]
    block = pieces[0].shape[0] // 8
    for m, piece in enumerate(pieces):
        for k in range(4):
            at, a, b = 2 * k * block, (m * 4 + k) * block, (k * 4 + m) * block
            mine[a : a + block, :] = piece[at : at + block, :]
            theirs[b : b + block, :] = piece[at + block : at + 2 * block, :]


def plane_of(pieces):
    rows, cols = pieces[0].shape
    return pl.pallas_call(
        plane_body,
        out_shape=[jax.ShapeDtypeStruct((2 * rows, cols), BF16)] * 2,
        in_specs=[vmem()] * 4,
        out_specs=[vmem()] * 2,
        compiler_params=LIMIT,
    )(*pieces)


def sum_body(total, s1, s2, s3, *pieces):
    rows = pieces[0].shape[0]
    for k, out in enumerate(pieces):
        at = slice(k * rows, (k + 1) * rows)
        value = total[at, :]
        for piece in (s1, s2, s3):
            value = value + piece[at, :].astype(F32)
        out[...] = value.astype(out.dtype)


def sum_of(total, sent):
    rows, cols = total.shape
    shape = (rows // 4, cols)
    return pl.pallas_call(
        sum_body,
        out_shape=[jax.ShapeDtypeStruct(shape, F32)] + [jax.ShapeDtypeStruct(shape, BF16)] * 3,
        in_specs=[vmem()] * 4,
        out_specs=[vmem()] * 4,
        compiler_params=LIMIT,
    )(total, *sent)


def last_body(*refs):
    ours, others = refs[-2:]
    rows, width = ours.shape[0] // 2, ours.shape[1]
    for half in range(2):
        own, *sent = refs[4 * half : 4 * half + 4]
        value = own[...]
        for piece in sent:
            value = value + piece[...].astype(F32)
        at = slice(half * rows, (half + 1) * rows)
        ours[at, :] = value[:, :width]
        others[at, :] = value[:, width:]


def last_of(even, odd):
    rows, cols = even[0].shape
    return pl.pallas_call(
        last_body,
        out_shape=[jax.ShapeDtypeStruct((2 * rows, cols // 2), F32)] * 2,
        in_specs=[vmem()] * 8,
        out_specs=[vmem()] * 2,
        compiler_params=LIMIT,
    )(*even, *odd)


def result_body(place, tokens, ours, others, bias, out):
    hold, width = tokens.shape[0], ours.shape[1]
    biases = row_of_tiles(bias[...])
    for zl in range(2):
        for c in range(2):

            @pl.when(place[0] == 2 * zl + c)
            def _():
                for half in range(2):
                    for ref, core in ((ours, c), (others, 1 - c)):
                        k = 2 * (zl ^ half) + core
                        at = slice(k * width, (k + 1) * width)
                        value = tokens[:, at].astype(F32) + ref[half * hold : (half + 1) * hold, :]
                        out[:, at] = (value + biases[:, at]).astype(BF16)


def result_of(place, tokens, ours, others, bias):
    return pl.pallas_call(
        result_body,
        out_shape=jax.ShapeDtypeStruct(tokens.shape, BF16),
        in_specs=[pl.BlockSpec(memory_space=pltpu.SMEM)] + [vmem()] * 4,
        out_specs=vmem(),
        compiler_params=LIMIT,
    )(place, tokens, ours, others, bias.reshape(-1, 128))


def ring(own, name):
    got = {0: own, 1: towards(own), -1: away(own)}
    for k in (2, 3):
        got[k] = towards(got[1 - k])
        got[-k] = away(got[k - 1])
    if name == "in":
        got[4] = towards(got[-3])
    else:
        got[4] = away(got[3])
    return got


def block(tokens, norm_gain, norm_bias, w_in, b_in, w_out, b_out):
    width = w_in.shape[0]
    near_in = ring(w_in, "in")
    place = (2 * lax.axis_index("zl") + lax.axis_index("c")).astype(jnp.int32).reshape(1)
    ours, others, joined = prologue_of(place, tokens, norm_gain, norm_bias, w_out.T, b_in)
    near_out = ring(joined, "out")
    far_in = {k: other_core(v) for k, v in near_in.items()}
    groups = ((0, 1), (-2, -1), (2, 3), (4, -3))

    both = jnp.concatenate([ours, other_core(others)], 0)
    row = row_of([both] + [from_step(both, 0, k) for k in (1, 2, 3)])
    mine, theirs = plane_of([row] + [from_step(row, 1, k) for k in (1, 2, 3)])
    theirs = other_core(theirs)

    own_h = []
    for i, (e, o) in enumerate(groups):
        before = (mine, near_in[e], near_in[o])
        if i < 3:
            before = (pre_of(*before),)
        bias = near_out[min(e, o, key=abs)]
        own_h.append(hidden_of(theirs, far_in[e], far_in[o], bias, *before))
    far_h = [other_core(h) for h in own_h]
    halves = [None] * 2
    for which, name, stage in ((1, "odd", 0), (0, "even", 1)):
        weights = [near_out[pair[which]] for pair in groups]
        if name == "odd":
            part = part_of(own_h[:3], far_h[:3], weights[:3], width)
            total, *sent = terms_of(own_h[3:], far_h[3:], weights[3:], width, stage, part)
        else:
            total, *sent = terms_of(own_h, far_h, weights, width, stage)
        sent = [to_step(piece, stage, k + 1) for k, piece in enumerate(sent)]
        own, *sent = sum_of(total, sent)
        sent = [to_step(piece, 1 - stage, k + 1) for k, piece in enumerate(sent)]
        halves[which] = (own, *sent)
    ours, others = last_of(*halves)
    return result_of(place, tokens, ours, other_core(others), b_out)


def solution(mesh):
    torus = Mesh(mesh.devices.reshape(2, 2, 4, 4, 4), AXES)
    return jax.shard_map(
        block,
        mesh=torus,
        in_specs=(P((*DP, *MP), None), P(), P(), P(DP, MP), P(MP), P(MP, DP), P()),
        out_specs=P((*DP, *MP), None),
        check_vma=False,
    )
```
